256 devices in a mesh: tm: 8 (over x, y_lo), space: 32 (over z, y_hi, core).
Axes of the slice: x: 4, y: 4 (y_hi: 2, y_lo: 2; y = y_hi * 2 + y_lo), z: 8, core: 2. Of those that a mesh axis runs over, the one named last changes fastest.
Arguments:
- source: float32 [16, 4096, 5, 128], P('tm', 'space'), may hold values from -6 to 6
- terminal: float32 [4096, 5, 128], P('space'), may hold values from -6 to 6
- jacobian: float32 [8, 4096, 5, 5, 128], P('tm', 'space')
- face_coef: float32 [4096, 6, 128], P('space'), may hold values from 0.1 to 0.5
- cell_coef: float32 [4096, 128], P('space'), may hold values from 0.1 to 0.5
- neighbours: int32 [4096, 6], P('space'), may hold values from 0 to 160, as said below
- send_blocks: int32 [32, 2, 16], P('space'), may hold values from 0 to 127, as said below
- live_count: int32 [32], P('space'), may hold values from 64 to 128, as said below
- volume: float32 [4096, 128], P('space'), may hold values from 0.5 to 2
- shape_field: float32 [4096, 5, 128], P('space'), may hold values from -6 to 6
- weights: float32 [16], P('tm'), may hold values from 0.25 to 4
Outputs:
- adjoint: float32 [16, 4096, 5, 128], P('tm', 'space')
- sensitivity: float32 [4096], P('space')
The draws below stay inside these ranges and needn't reach their ends.
Inputs may be any that keep to these rules, and one draw needn't show every extreme that they name: `live_count`: some device has 128 live blocks in every draw. `send_blocks`: each index names a live block of its own device. `neighbours`: a slot below 128 names a live block of the same device; 128 to 159 name received blocks, those of the lower device first; 160 is an empty slot.
All inputs are finite; a program needn't handle non-finite values.
Results may differ from the reference program's by a relative error of at most 0.00016.
Values sent between devices are 32-bit elements; how exact they have to be, the bound alone decides.
A program may use at most 64 MiB of HBM per device.

```python
import math
import jax
import jax.numpy as jnp
from jax import lax

NB = 128
CELLS = 128
COMP = 5
NEI = 6
HALO = 16
STEPS = 2
ITERS = 3
BLOCKS = 4096
GROUPS = 8
TSTEPS = 16
N_SPACE = 32


def geometry(key):
    devices = BLOCKS // NB
    keys = jax.random.split(jax.random.fold_in(key, 17), 6)
    counts = jax.random.randint(keys[0], (devices,), NB // 2, NB + 1)
    fullest = jax.random.randint(keys[1], (), 0, devices)
    counts = counts.at[fullest].set(NB)
    sends = jax.random.randint(keys[2], (devices, 2, HALO), 0, 1 << 20) % counts[:, None, None]
    kinds = jax.random.randint(keys[3], (BLOCKS, NEI), 0, 6)
    block_counts = jnp.repeat(counts, NB)
    local = jax.random.randint(keys[4], (BLOCKS, NEI), 0, 1 << 20) % block_counts[:, None]
    remote = NB + jax.random.randint(keys[5], (BLOCKS, NEI), 0, 2 * HALO)
    table = jnp.where(kinds < 2, remote, jnp.where(kinds == 2, NB + 2 * HALO, local))
    return (counts.astype(jnp.int32), sends.astype(jnp.int32), table.astype(jnp.int32))


def draw_live_count(key, part):
    return geometry(key)[0]


def draw_send_blocks(key, part):
    return geometry(key)[1]


def draw_neighbours(key, part):
    return geometry(key)[2]


def draw_jacobian(key, part):
    first, second = jax.random.split(jax.random.fold_in(key, 29))
    shape = (GROUPS, BLOCKS, COMP, COMP, CELLS)
    identity = jnp.eye(COMP, dtype=jnp.float32)[None, None, :, :, None]
    off_part = 0.15 * jax.random.normal(first, shape, jnp.float32)
    diag_part = jax.random.uniform(second, shape, jnp.float32, 0.3, 1.0)
    return identity * diag_part + (1.0 - identity) * off_part


def block_scale(stream_key, shape, shards, smallest, top_value):
    gain, own = 1.0, jax.random.fold_in(stream_key, 6)
    for dim, shards_of in shards:
        draws = jnp.exp(jax.random.uniform(jax.random.fold_in(own, dim), (shards_of,), jnp.float32, smallest / len(shards), top_value / len(shards)))
        gain = gain * jnp.repeat(draws, shape[dim] // shards_of).reshape([-1 if axis == dim else 1 for axis in range(len(shape))])
    return gain


def scatter_about(stream_key, dims, spread, limit, cuts=(), kind=jnp.bfloat16):
    entries = spread * jax.random.normal(stream_key, dims, jnp.float32)
    if cuts:
        entries = entries * block_scale(stream_key, dims, cuts, -0.22, 0.18)
    return jnp.clip(entries, -limit, limit).astype(kind)


def setup_inputs(seed: int = 0) -> dict:
    arg_keys = jax.random.split(jax.random.key(seed), 12)
    source = scatter_about(arg_keys[0], (TSTEPS, BLOCKS, COMP, CELLS), 1.0, 6.0, ((0, 8), (1, 32)), jnp.float32)
    terminal = scatter_about(arg_keys[1], (BLOCKS, COMP, CELLS), 1.0, 6.0, ((0, 32),), jnp.float32)
    jacobian = draw_jacobian(jax.random.fold_in(arg_keys[11], 71), 0)
    face_coef = jnp.clip(0.1 + 0.4 * jax.random.uniform(arg_keys[3], (BLOCKS, NEI, CELLS), jnp.float32) ** block_scale(arg_keys[3], (BLOCKS, NEI, CELLS), ((0, 32),), -0.2, 0.2), 0.1, 0.5)
    cell_coef = jnp.clip(0.1 + 0.4 * jax.random.uniform(arg_keys[4], (BLOCKS, CELLS), jnp.float32) ** block_scale(arg_keys[4], (BLOCKS, CELLS), ((0, 32),), -0.2, 0.2), 0.1, 0.5)
    neighbours = draw_neighbours(jax.random.fold_in(arg_keys[11], 71), 0)
    send_blocks = draw_send_blocks(jax.random.fold_in(arg_keys[11], 71), 0)
    live_count = draw_live_count(jax.random.fold_in(arg_keys[11], 71), 0)
    volume = jnp.clip(jnp.exp(math.log(2.0) - 1.3862944 * jax.random.uniform(arg_keys[8], (BLOCKS, CELLS), jnp.float32) ** block_scale(arg_keys[8], (BLOCKS, CELLS), ((0, 32),), -0.2, 0.2)), 0.5, 2.0)
    shape_field = scatter_about(arg_keys[9], (BLOCKS, COMP, CELLS), 1.0, 6.0, ((0, 32),), jnp.float32)
    weights = jnp.clip(jnp.exp(math.log(4.0) - 2.7725887 * jax.random.uniform(arg_keys[10], (TSTEPS,), jnp.float32) ** block_scale(arg_keys[10], (TSTEPS,), ((0, 8),), -0.2, 0.2)), 0.25, 4.0)
    return {"source": source, "terminal": terminal, "jacobian": jacobian, "face_coef": face_coef, "cell_coef": cell_coef, "neighbours": neighbours, "send_blocks": send_blocks, "live_count": live_count, "volume": volume, "shape_field": shape_field, "weights": weights}


inverse_step = 6.0


def pick_rows(table, index):
    return table[index]


def reference(source, terminal, jacobian, face_coef, cell_coef, neighbours, send_blocks, live_count, volume, shape_field, weights):
    highest = lax.Precision.HIGHEST
    live = (jnp.arange(NB, dtype=jnp.int32)[None, :] < live_count[:, None]).astype(jnp.float32).reshape(BLOCKS, 1, 1)
    mass = (inverse_step * volume)[:, None, :]
    face_total = jnp.sum(face_coef, axis=1)[:, None, :]
    along_coef = cell_coef[:, None, :]
    neighbour_table = neighbours.reshape(N_SPACE, NB, NEI)

    def operate(field, jac):
        by_device = field.reshape(N_SPACE, NB, COMP, CELLS)
        to_lower = jax.vmap(pick_rows)(by_device, send_blocks[:, 0])
        to_higher = jax.vmap(pick_rows)(by_device, send_blocks[:, 1])
        zero_rim = jnp.zeros((1, HALO, COMP, CELLS), jnp.float32)
        from_lower = jnp.concatenate([zero_rim, to_higher[:-1]], axis=0)
        from_higher = jnp.concatenate([to_lower[1:], zero_rim], axis=0)
        blank = jnp.zeros((N_SPACE, 1, COMP, CELLS), jnp.float32)
        extended = jnp.concatenate([by_device, from_lower, from_higher, blank], axis=1)
        gathered = jax.vmap(pick_rows)(extended, neighbour_table).reshape(BLOCKS, NEI, COMP, CELLS)
        coupled = jnp.einsum("bnc,bnkc->bkc", face_coef, gathered, precision=highest)
        own = jnp.einsum("bijc,bic->bjc", jac, field, precision=highest)
        padded = jnp.pad(field, ((0, 0), (0, 0), (1, 1)))
        beside = padded[:, :, :-2] + padded[:, :, 2:]
        return mass * field + own - coupled - along_coef * beside

    later = live * terminal
    levels = []
    sensitivity = jnp.zeros((BLOCKS,), jnp.float32)
    for group in reversed(range(GROUPS)):
        jac = jacobian[group]
        diagonal = jnp.stack([jac[:, k, k, :] for k in range(COMP)], axis=1)
        precond = 1.0 / (mass + diagonal + face_total + 2.0 * along_coef)
        for level in reversed(range(STEPS)):
            index = group * STEPS + level
            rhs = source[index] + mass * later
            field = later
            for sweep in range(ITERS):
                field = live * (field + precond * (rhs - operate(field, jac)))
            levels.append(field)
            sensitivity = sensitivity + weights[index] * jnp.sum(field * shape_field, axis=(1, 2))
            later = field
    adjoint = jnp.stack(levels[::-1], axis=0)
    return adjoint, sensitivity
```

```python
import functools

import jax
import jax.numpy as jnp
from jax import lax
from jax.experimental import pallas as pl
from jax.experimental.pallas import tpu as pltpu
from jax.sharding import PartitionSpec as P

ITERS = 3
STEPS = 2
SWEEPS = ITERS * STEPS
SLOTS = 3
CHUNKS = 4
INVERSE_STEP = 6.0
MESH = pl.DeviceIdType.MESH
F32 = jnp.float32


def kernel(
    src_h, term_h, jac_h, face_h, cell_h, nbr, snd, live_s, vol_h, shape_h, w_s,
    adj_o, sens_o,
    K, SRC, F, CL, CR, VOL, SH, LP, LPM, R, XIN, XB, YB, CB, LPB, E0, E1, E2,
    SLO, SHI, OUT, ACC, RED, PART, TOT,
    ld, xr, elo, ehi, slo, shi, osem, hsem, psr, pss, fss, fsr,
):
    comp, nb, cells = XIN.shape
    nei = F.shape[0]
    halo = SLO.shape[1]
    groups = nb // 8
    tm = lax.axis_index("tm")
    d = lax.axis_index("space")
    n_tm = lax.axis_size("tm")
    n_sp = lax.axis_size("space")
    has_lo, has_hi = d > 0, d < n_sp - 1
    first, last = tm == n_tm - 1, tm == 0
    E = (E0, E1, E2)
    lo, hi = d - 1, d + 1
    XR, YR, CRW, LPR = (ref.reshape(ref.shape[0] * 8, cells) for ref in (XB, YB, CB, LPB))

    loads = [
        pltpu.make_async_copy(jac_h.at[0], K, ld.at[0]),
        pltpu.make_async_copy(face_h, F, ld.at[1]),
        pltpu.make_async_copy(cell_h, CL, ld.at[2]),
        pltpu.make_async_copy(vol_h, VOL, ld.at[3]),
        pltpu.make_async_copy(src_h, SRC, ld.at[4]),
        pltpu.make_async_copy(shape_h, SH, ld.at[5]),
    ]
    for copy in loads:
        copy.start()
    term_copy = pltpu.make_async_copy(term_h, XIN, ld.at[6])

    @pl.when(first)
    def _():
        term_copy.start()

    barrier = pltpu.get_barrier_semaphore()
    for dt in (-1, 0, 1):
        for ds in (-1, 0, 1):
            if dt == 0 and ds == 0:
                continue
            ok = jnp.logical_and(
                jnp.logical_and(tm + dt >= 0, tm + dt < n_tm),
                jnp.logical_and(d + ds >= 0, d + ds < n_sp),
            )

            @pl.when(ok)
            def _():
                pl.semaphore_signal(barrier, 1, device_id=(tm + dt, d + ds), device_id_type=MESH)

    @pl.when(last)
    def _():
        for row in range(2, n_tm):
            pl.semaphore_signal(barrier, 1, device_id=(row, d), device_id_type=MESH)

    @pl.when(tm >= 2)
    def _():
        pl.semaphore_signal(barrier, 1, device_id=(0, d), device_id_type=MESH)

    zero = jnp.zeros((comp, cells), F32)
    for e in E:

        def clear(i, _):
            for u in range(8):
                e[i * 8 + u] = zero
            return 0

        lax.fori_loop(0, nb // 8, clear, 0)
        e[nb + 2 * halo] = zero

        @pl.when(jnp.logical_not(has_lo))
        def _():
            for s in range(halo):
                e[nb + s] = zero

        @pl.when(jnp.logical_not(has_hi))
        def _():
            for s in range(halo):
                e[nb + halo + s] = zero

    for s in range(2 * halo + 1):
        XB[nb + s] = jnp.zeros((8, cells), F32)

    for copy in loads[:4]:
        copy.wait()

    lc = live_s[0]
    lane = lax.broadcasted_iota(jnp.int32, (8, cells), 1)
    sub = lax.broadcasted_iota(jnp.int32, (8, cells), 0)

    def prepare(g, _):
        rows = pl.ds(pl.multiple_of(g * 8, 8), 8)
        mass = INVERSE_STEP * VOL[rows, :]
        cell = CL[rows, :]
        fsum = F[0, rows, :]
        for k in range(1, nei):
            fsum = fsum + F[k, rows, :]
        CR[rows, :] = jnp.where(lane == cells - 1, 0.0, cell)
        CL[rows, :] = jnp.where(lane == 0, 0.0, cell)
        live = jnp.where(sub + g * 8 < lc, 1.0, 0.0)
        for j in range(comp):
            lp = live / (mass + K[j, j, rows, :] + fsum + 2.0 * cell)
            lpm = lp * mass
            LP[j, rows, :] = lp
            LPM[j, rows, :] = lpm
            LPR[pl.ds(g * 64 + j, 8, stride=8), :] = lp
            for i in range(comp):
                k_ij = -lp * K[i, j, rows, :]
                if i == j:
                    k_ij = k_ij + (live - lpm)
                K[i, j, rows, :] = k_ij
        return 0

    lax.fori_loop(0, groups, prepare, 0)

    partners = (
        jnp.where(has_lo, 1, 0) + jnp.where(has_hi, 1, 0)
    )
    rows_near = jnp.where(first, 0, 1) + jnp.where(last, 0, 1)
    expect = partners + rows_near * (1 + partners)
    expect = expect + jnp.where(last, n_tm - 2, 0) + jnp.where(tm >= 2, 1, 0)
    pl.semaphore_wait(barrier, expect)

    def halo_copy(side, slot, buf, row):
        if side == 0:
            return pltpu.make_async_remote_copy(
                SLO.at[buf], E[slot].at[pl.ds(nb + halo, halo)], slo.at[buf], ehi.at[slot],
                device_id=(row, lo), device_id_type=MESH)
        return pltpu.make_async_remote_copy(
            SHI.at[buf], E[slot].at[pl.ds(nb, halo)], shi.at[buf], elo.at[slot],
            device_id=(row, hi), device_id_type=MESH)

    def start_side(side, slot, buf, row, cond):
        @pl.when(cond)
        def _():
            halo_copy(side, slot, buf, row).start()

    def state_copy(c):
        rows = pl.ds(c * (nb // CHUNKS), nb // CHUNKS)
        return pltpu.make_async_remote_copy(
            OUT.at[0, :, rows], XIN.at[:, rows], hsem.at[c], xr.at[c],
            device_id=(tm - 1, d), device_id_type=MESH)

    @pl.when(first)
    def _():
        term_copy.wait()

    @pl.when(jnp.logical_not(first))
    def _():
        for c in range(CHUNKS):
            state_copy(c).wait_recv()

    def spread(g, _):
        rows = pl.ds(pl.multiple_of(g * 8, 8), 8)
        keep = jnp.where(sub + g * 8 < lc, 1.0, 0.0)
        for j in range(comp):
            XR[pl.ds(g * 64 + j, 8, stride=8), :] = keep * XIN[j, rows, :]
        return 0

    lax.fori_loop(0, groups, spread, 0)

    @pl.when(first)
    def _():
        for side, buf in ((0, SLO), (1, SHI)):
            for s in range(halo):
                buf[1, s] = XB[snd[side, s]][:comp]
        start_side(0, 0, 1, tm, has_lo)
        start_side(1, 0, 1, tm, has_hi)

    loads[4].wait()
    loads[5].wait()

    for it in range(SWEEPS):
        level = STEPS - 1 - it // ITERS
        sweep = it % ITERS
        slot = it % SLOTS
        buf = it % 2

        def gather_local(g, _):
            for u in range(8):
                b = g * 8 + u
                c = None
                for k in range(nei):
                    t = F[k, pl.ds(b, 1), :] * XB[nbr[k, b]]
                    c = t if c is None else c + t
                CB[b] = c
            return 0

        lax.fori_loop(0, groups, gather_local, 0)

        def own(g, _):
            rows = pl.ds(pl.multiple_of(g * 8, 8), 8)
            xs = [XR[pl.ds(g * 64 + j, 8, stride=8), :] for j in range(comp)]
            cl, cr = CL[rows, :], CR[rows, :]
            for j in range(comp):
                lp = LP[j, rows, :]
                if sweep == 0:
                    y = lp * SRC[level, j, rows, :] + LPM[j, rows, :] * xs[j]
                    R[j, rows, :] = y
                else:
                    y = R[j, rows, :]
                for i in range(comp):
                    y = y + K[i, j, rows, :] * xs[i]
                beside = cl * pltpu.roll(xs[j], 1, 1) + cr * pltpu.roll(xs[j], cells - 1, 1)
                y = y + lp * (CRW[pl.ds(g * 64 + j, 8, stride=8), :] + beside)
                YR[pl.ds(g * 64 + j, 8, stride=8), :] = y
            return 0

        lax.fori_loop(0, groups, own, 0)

        if it >= 2:
            @pl.when(has_lo)
            def _():
                halo_copy(0, 0, buf, tm).wait_send()

            @pl.when(has_hi)
            def _():
                halo_copy(1, 0, buf, tm).wait_send()
        if it == 1:
            @pl.when(jnp.logical_and(first, has_lo))
            def _():
                halo_copy(0, 0, buf, tm).wait_send()

            @pl.when(jnp.logical_and(first, has_hi))
            def _():
                halo_copy(1, 0, buf, tm).wait_send()

        @pl.when(has_hi)
        def _():
            halo_copy(0, slot, buf, tm).wait_recv()

        @pl.when(has_lo)
        def _():
            halo_copy(1, slot, buf, tm).wait_recv()

        e = E[slot]

        def finish(b):
            c = None
            for k in range(nei):
                t = F[k, b][None, :] * e[nbr[k, b]]
                c = t if c is None else c + t
            return YB[b][:comp] + LPB[b][:comp] * c

        final = it == SWEEPS - 1
        if final:
            row, after = tm - 1, 0
            go_lo = jnp.logical_and(has_lo, jnp.logical_not(last))
            go_hi = jnp.logical_and(has_hi, jnp.logical_not(last))
        else:
            row, after = tm, (it + 1) % SLOTS
            go_lo, go_hi = has_lo, has_hi
        for side, store, go in ((0, SLO, go_lo), (1, SHI, go_hi)):
            for s in range(halo):
                store[buf, s] = finish(snd[side, s])
            start_side(side, after, buf, row, go)

        def post(g, _):
            for u in range(8):
                b = g * 8 + u
                XB[b, pl.ds(0, comp), :] = finish(b)
            return 0

        if sweep < ITERS - 1:
            lax.fori_loop(0, groups, post, 0)
            continue

        w = w_s[level]

        def post_level(g, _):
            post(g, 0)
            rows = pl.ds(pl.multiple_of(g * 8, 8), 8)
            acc = None
            for j in range(comp):
                x = XR[pl.ds(g * 64 + j, 8, stride=8), :]
                OUT[level, j, rows, :] = x
                t = x * SH[j, rows, :]
                acc = t if acc is None else acc + t
            acc = w * acc
            if it > ITERS:
                acc = ACC[rows, :] + acc
            ACC[rows, :] = acc
            return 0

        if not final:
            lax.fori_loop(0, groups, post_level, 0)
        else:
            for c in range(CHUNKS):
                lax.fori_loop(c * groups // CHUNKS, (c + 1) * groups // CHUNKS, post_level, 0)

                @pl.when(jnp.logical_not(last))
                def _():
                    state_copy(c).start()

        pltpu.make_async_copy(OUT.at[level], adj_o.at[level], osem.at[level]).start()

    PART[...] = jnp.sum(ACC[...].T, axis=0, keepdims=True)

    def part_copy():
        return pltpu.make_async_remote_copy(
            PART, RED, pss, psr, device_id=(tm - 1, d), device_id_type=MESH)

    @pl.when(jnp.logical_not(first))
    def _():
        part_copy().wait_recv()
        PART[...] = PART[...] + RED[...]

    @pl.when(jnp.logical_not(last))
    def _():
        part_copy().start()

    def total_copy(row):
        return pltpu.make_async_remote_copy(
            PART, TOT, fss.at[row], fsr, device_id=(row, d), device_id_type=MESH)

    @pl.when(last)
    def _():
        for row in range(1, n_tm):
            total_copy(row).start()
        sens_o[...] = PART[...]
        for row in range(1, n_tm):
            total_copy(row).wait_send()

    @pl.when(jnp.logical_not(last))
    def _():
        for c in range(CHUNKS):
            state_copy(c).wait_send()
        part_copy().wait_send()
        total_copy(0).wait_recv()
        sens_o[...] = TOT[...]

    inner = (SWEEPS - 2) % 2
    outer = (SWEEPS - 1) % 2
    for side, has in ((0, has_lo), (1, has_hi)):
        @pl.when(has)
        def _():
            halo_copy(side, 0, inner, tm).wait_send()

        @pl.when(jnp.logical_and(has, jnp.logical_not(last)))
        def _():
            halo_copy(side, 0, outer, tm).wait_send()
    for level in range(STEPS):
        pltpu.make_async_copy(OUT.at[level], adj_o.at[level], osem.at[level]).wait()


def per_device(source, terminal, jacobian, face_coef, cell_coef, neighbours, send_blocks,
               live_count, volume, shape_field, weights):
    nb, comp, cells = terminal.shape
    nei = face_coef.shape[1]
    halo = send_blocks.shape[2]
    anys = pl.BlockSpec(memory_space=pl.ANY)
    smem = pl.BlockSpec(memory_space=pltpu.SMEM)
    vmem = pltpu.VMEM
    dma = pltpu.SemaphoreType.DMA
    table = nb + 2 * halo + 1
    adj, sens = pl.pallas_call(
        kernel,
        out_shape=(
            jax.ShapeDtypeStruct((STEPS, comp, nb, cells), F32),
            jax.ShapeDtypeStruct((1, nb), F32),
        ),
        in_specs=[anys, anys, anys, anys, anys, smem, smem, smem, anys, anys, smem],
        out_specs=(anys, pl.BlockSpec(memory_space=pltpu.VMEM)),
        scratch_shapes=[
            vmem((comp, comp, nb, cells), F32),
            vmem((STEPS, comp, nb, cells), F32),
            vmem((nei, nb, cells), F32),
            vmem((nb, cells), F32),
            vmem((nb, cells), F32),
            vmem((nb, cells), F32),
            vmem((comp, nb, cells), F32),
            vmem((comp, nb, cells), F32),
            vmem((comp, nb, cells), F32),
            vmem((comp, nb, cells), F32),
            vmem((comp, nb, cells), F32),
            vmem((table, 8, cells), F32),
            vmem((nb, 8, cells), F32),
            vmem((nb, 8, cells), F32),
            vmem((nb, 8, cells), F32),
            vmem((table, comp, cells), F32),
            vmem((table, comp, cells), F32),
            vmem((table, comp, cells), F32),
            vmem((2, halo, comp, cells), F32),
            vmem((2, halo, comp, cells), F32),
            vmem((STEPS, comp, nb, cells), F32),
            vmem((nb, cells), F32),
            vmem((1, nb), F32),
            vmem((1, nb), F32),
            vmem((1, nb), F32),
            dma((7,)),
            dma((CHUNKS,)),
            dma((SLOTS,)),
            dma((SLOTS,)),
            dma((2,)),
            dma((2,)),
            dma((STEPS,)),
            dma((CHUNKS,)),
            dma(()),
            dma(()),
            dma((lax.axis_size("tm"),)),
            dma(()),
        ],
        compiler_params=pltpu.CompilerParams(collective_id=0, has_side_effects=True),
        name="sweep",
    )(
        source.transpose(0, 2, 1, 3),
        terminal.transpose(1, 0, 2),
        jacobian.transpose(0, 2, 3, 1, 4),
        face_coef.transpose(1, 0, 2),
        cell_coef,
        neighbours.T,
        send_blocks[0],
        live_count,
        volume,
        shape_field.transpose(1, 0, 2),
        weights,
    )
    return adj.transpose(0, 2, 1, 3), sens.reshape(nb)


def solution(mesh):
    return jax.shard_map(
        per_device,
        mesh=mesh,
        in_specs=(
            P("tm", "space", None, None),
            P("space", None, None),
            P("tm", "space", None, None, None),
            P("space", None, None),
            P("space", None),
            P("space", None),
            P("space", None, None),
            P("space"),
            P("space", None),
            P("space", None, None),
            P("tm"),
        ),
        out_specs=(P("tm", "space", None, None), P("space")),
        check_vma=False,
    )
```

```python
import functools

import jax
import jax.numpy as jnp
from jax import lax
from jax.experimental import pallas as pl
from jax.experimental.pallas import tpu as pltpu
from jax.sharding import PartitionSpec as P

ITERS = 3
STEPS = 2
SWEEPS = ITERS * STEPS
SLOTS = 3
CHUNKS = 4
PIECES = 3
INVERSE_STEP = 6.0
MESH = pl.DeviceIdType.MESH
F32 = jnp.float32


def both(*conds):
    return functools.reduce(jnp.logical_and, conds)


def kernel(
    src_h, term_h, jac_h, face_h, cell_h, ints_h, vol_h, shape_h, w_s,
    adj_o, sens_o,
    KA, KB, SRCA, SRCB, F, CELL, CL, CR, VOL, SH, LPA, LPB, LPMA, LPMB, LBA, LBB,
    R, XIN, XB, YB, E0, E1, E2, SLO, SHI, OUTA, OUTB, ACC, RED, PART, TOT,
    WOUT, WA, WB, IV, INTS, FH, LHA, LHB, NH,
    ra, rb, sa, rc, sc, isem, xr, elo, ehi, slo, shi, oas, obs, ors, hsem, psr, pss, fss, fsr,
):
    comp, nb, cells = XIN.shape
    nei = F.shape[0]
    halo = SLO.shape[1]
    groups = nb // 8
    tm = lax.axis_index("tm")
    d = lax.axis_index("space")
    n_tm = lax.axis_size("tm")
    n_sp = lax.axis_size("space")

    x, z, c = tm // 2, d // 4, d % 2
    y = (d // 2) % 2 * 2 + tm % 2

    def path(k, q):
        qz, j = q // 4, q % 4
        qy = jnp.where(qz % 2 == 0, j, 3 - j)
        return 2 * k + qy % 2, 4 * qz + qy // 2 * 2 + 1

    n_planes = n_tm // 2
    native = x == n_planes - 1
    onpath = both(jnp.logical_not(native), c == 1)
    active = jnp.logical_or(native, onpath)
    p = jnp.where(native, d, 4 * z + jnp.where(z % 2 == 0, y, 3 - y))
    first = tm == n_tm - 1
    last = both(onpath, x == 0)
    more = both(active, jnp.logical_not(last))
    later = both(active, jnp.logical_not(first))
    has_lo, has_hi = p > 0, p < n_sp - 1

    def pick(cond, a, b):
        return jnp.where(cond, a[0], b[0]), jnp.where(cond, a[1], b[1])

    def same(dev):
        return both(dev[0] == tm, dev[1] == d)

    def peer(q):
        return pick(native, (tm, q), path(x, q))

    def next_dev(q):
        return pick(first, (tm - 1, q), pick(native, path(x - 1, q), path(jnp.maximum(x - 1, 0), q)))

    def prev_dev(q):
        return pick(native, (tm + 1, q), pick(x == n_planes - 2, (n_tm - 2, q), path(x + 1, q)))

    lo, hi = peer(p - 1), peer(p + 1)
    nxt = next_dev(p)
    nlo, nhi = next_dev(p - 1), next_dev(p + 1)
    home_a, home_b = (2 * x + 1, p), (2 * x, p)
    self_a = same(home_a)
    mover = jnp.logical_not(native)
    worker = path(x, d)
    own_worker = same(worker)
    odd = tm % 2 == 1
    summer = path(0, d)
    own_summer = same(summer)

    def remote(src, dst, ssem, rsem, dev):
        return pltpu.make_async_remote_copy(src, dst, ssem, rsem, device_id=dev, device_id_type=MESH)

    local = [
        pltpu.make_async_copy(face_h, F, rc.at[0]),
        pltpu.make_async_copy(cell_h, CELL, rc.at[1]),
        pltpu.make_async_copy(vol_h, VOL, rc.at[2]),
        pltpu.make_async_copy(shape_h, SH, rc.at[3]),
        pltpu.make_async_copy(ints_h, INTS, isem),
        pltpu.make_async_copy(jac_h.at[0], KB, rb.at[0]),
        pltpu.make_async_copy(src_h, SRCB, rb.at[1]),
    ]

    @pl.when(native)
    def _():
        for copy in local:
            copy.start()

    term_copy = pltpu.make_async_copy(term_h, XIN, xr.at[0])

    @pl.when(first)
    def _():
        term_copy.start()

    barrier = pltpu.get_barrier_semaphore()
    edges = [(both(active, has_lo), lo), (both(active, has_hi), hi)]
    for ds in (-1, 0, 1):
        inside = both(p + ds >= 0, p + ds < n_sp)
        edges.append((both(more, inside), next_dev(p + ds)))
        edges.append((both(later, inside), prev_dev(p + ds)))
    edges.append((both(mover, jnp.logical_not(own_worker)), worker))
    edges.append((both(onpath, jnp.logical_not(self_a)), home_a))
    edges.append((onpath, home_b))
    for t in range(n_tm):
        edges.append((both(last, jnp.logical_not(same((t, p)))), (t, p)))
    edges.append((jnp.logical_not(own_summer), summer))
    expect = 0
    for cond, dev in edges:

        @pl.when(cond)
        def _():
            pl.semaphore_signal(barrier, 1, device_id=dev, device_id_type=MESH)

        expect = expect + jnp.where(cond, 1, 0)

    for level in range(STEPS):
        WOUT[level] = jnp.full((1, cells), w_s[level], F32)

        @pl.when(native)
        def _():
            WB[level] = jnp.full((1, cells), w_s[level], F32)

    pl.semaphore_wait(barrier, expect)

    def coefficients(dev):
        return [
            remote(ints_h, IV, sc.at[4], rc.at[4], dev),
            remote(face_h, F, sc.at[0], rc.at[0], dev),
            remote(cell_h, CELL, sc.at[1], rc.at[1], dev),
            remote(vol_h, VOL, sc.at[2], rc.at[2], dev),
            remote(shape_h, SH, sc.at[3], rc.at[3], dev),
        ]

    def slab_operands(K, SRC, W, sems, dev):
        return [
            remote(jac_h.at[0], K, sa.at[0], sems.at[0], dev),
            remote(src_h, SRC, sa.at[1], sems.at[1], dev),
            remote(WOUT, W, sa.at[2], sems.at[2], dev),
        ]

    self_operands = [
        pltpu.make_async_copy(jac_h.at[0], KA, ra.at[0]),
        pltpu.make_async_copy(src_h, SRCA, ra.at[1]),
    ]

    @pl.when(both(mover, odd, jnp.logical_not(own_worker)))
    def _():
        for copy in slab_operands(KA, SRCA, WA, ra, worker):
            copy.start()

    @pl.when(both(mover, odd, own_worker))
    def _():
        for copy in self_operands:
            copy.start()
        WA[...] = WOUT[...]

    @pl.when(both(mover, jnp.logical_not(odd)))
    def _():
        for copy in coefficients(worker):
            copy.start()
        for copy in slab_operands(KB, SRCB, WB, rb, worker):
            copy.start()

    E = (E0, E1, E2)
    XR, YR, LAR, LBR = (ref.reshape(ref.shape[0] * 8, cells) for ref in (XB, YB, LBA, LBB))
    lane = lax.broadcasted_iota(jnp.int32, (8, cells), 1)
    sub = lax.broadcasted_iota(jnp.int32, (8, cells), 0)
    sends = nei * nb

    def halo_copy(side, slot, buf, dev):
        if side == 0:
            return remote(SLO.at[buf], E[slot].at[pl.ds(nb + halo, halo)], slo.at[buf], ehi.at[slot], dev)
        return remote(SHI.at[buf], E[slot].at[pl.ds(nb, halo)], shi.at[buf], elo.at[slot], dev)

    def start_side(side, slot, buf, dev, cond):
        @pl.when(cond)
        def _():
            halo_copy(side, slot, buf, dev).start()

    def state_copy(i):
        rows = pl.ds(i * (nb // CHUNKS), nb // CHUNKS)
        return remote(OUTB.at[0, :, rows], XIN.at[:, rows], hsem.at[i], xr.at[i], nxt)

    def halo_tables():
        for s in range(2 * halo):
            b = INTS[sends + s]
            for k in range(nei):
                NH[s * nei + k] = INTS[k * nb + b]
                FH[k, pl.ds(s, 1), :] = F[k, b][None, :]

    def prepare_slab(K, LP, LPM, LB, LPR, LH):
        lc = INTS[sends + 2 * halo]

        def prepare(g, _):
            rows = pl.ds(pl.multiple_of(g * 8, 8), 8)
            mass = INVERSE_STEP * VOL[rows, :]
            cell = CELL[rows, :]
            fsum = F[0, rows, :]
            for k in range(1, nei):
                fsum = fsum + F[k, rows, :]
            CR[rows, :] = jnp.where(lane == cells - 1, 0.0, cell)
            CL[rows, :] = jnp.where(lane == 0, 0.0, cell)
            live = jnp.where(sub + g * 8 < lc, 1.0, 0.0)
            for j in range(comp):
                lp = live / (mass + K[j, j, rows, :] + fsum + 2.0 * cell)
                lpm = lp * mass
                LP[j, rows, :] = lp
                LPM[j, rows, :] = lpm
                LPR[pl.ds(g * 64 + j, 8, stride=8), :] = lp
                for i in range(comp):
                    k_ij = -lp * K[i, j, rows, :]
                    if i == j:
                        k_ij = k_ij + (live - lpm)
                    K[i, j, rows, :] = k_ij
            return 0

        lax.fori_loop(0, groups, prepare, 0)
        for s in range(2 * halo):
            LH[s] = LB[INTS[sends + s]]

    def spread(g, _):
        rows = pl.ds(pl.multiple_of(g * 8, 8), 8)
        keep = jnp.where(sub + g * 8 < INTS[sends + 2 * halo], 1.0, 0.0)
        for j in range(comp):
            XR[pl.ds(g * 64 + j, 8, stride=8), :] = keep * XIN[j, rows, :]
        for u in range(8):
            E0[g * 8 + u] = XB[g * 8 + u][:comp]
        return 0

    def start_state():
        term_copy.wait()
        lax.fori_loop(0, groups, spread, 0)
        for side, store in ((0, SLO), (1, SHI)):
            for s in range(halo):
                store[1, s] = XB[INTS[sends + side * halo + s]][:comp]
        start_side(0, 0, 1, lo, has_lo)
        start_side(1, 0, 1, hi, has_hi)

    def run_slab(K, SRC, LP, LPM, LB, LH, W, OUT, ends, began):
        for it in range(SWEEPS):
            level = STEPS - 1 - it // ITERS
            sweep = it % ITERS
            slot = it % SLOTS
            buf = it % 2

            def own(g, _):
                rows = pl.ds(pl.multiple_of(g * 8, 8), 8)
                xs = [XR[pl.ds(g * 64 + j, 8, stride=8), :] for j in range(comp)]
                cl, cr = CL[rows, :], CR[rows, :]
                for j in range(comp):
                    lp = LP[j, rows, :]
                    if sweep == 0:
                        v = lp * SRC[level, j, rows, :] + LPM[j, rows, :] * xs[j]
                        R[j, rows, :] = v
                    else:
                        v = R[j, rows, :]
                    for i in range(comp):
                        v = v + K[i, j, rows, :] * xs[i]
                    beside = cl * pltpu.roll(xs[j], 1, 1) + cr * pltpu.roll(xs[j], cells - 1, 1)
                    v = v + lp * beside
                    YR[pl.ds(g * 64 + j, 8, stride=8), :] = v
                return 0

            def spread_own(g, _):
                spread(g, 0)
                own(g, 0)
                return 0

            def arrive():
                for i in range(CHUNKS):
                    state_copy(i).wait_recv()
                    lax.fori_loop(i * groups // CHUNKS, (i + 1) * groups // CHUNKS, spread_own, 0)

            if it == 0 and not ends:
                arrive()
            elif it == 0:
                @pl.when(first)
                def _():
                    start_state()
                    lax.fori_loop(0, groups, own, 0)

                @pl.when(both(native, later))
                def _():
                    arrive()

                @pl.when(onpath)
                def _():
                    lax.fori_loop(0, groups, own, 0)
            else:
                lax.fori_loop(0, groups, own, 0)

            used = None
            if it >= 2:
                used = active
            elif ends:
                used = began if it == 0 else jnp.logical_or(began, first)
            if used is not None:
                for side, has in ((0, has_lo), (1, has_hi)):
                    @pl.when(both(used, has))
                    def _():
                        halo_copy(side, 0, buf, lo).wait_send()

            @pl.when(has_hi)
            def _():
                halo_copy(0, slot, buf, lo).wait_recv()

            @pl.when(has_lo)
            def _():
                halo_copy(1, slot, buf, hi).wait_recv()

            e, ahead = E[slot], E[(it + 1) % SLOTS]

            final = ends and it == SWEEPS - 1
            if final:
                to, after, go = (nlo, nhi), 0, more
            else:
                to, after, go = (lo, hi), (it + 1) % SLOTS, active
            for side, store, has in ((0, SLO, has_lo), (1, SHI, has_hi)):
                for s in range(halo):
                    at = side * halo + s
                    v = None
                    for k in range(nei):
                        t = FH[k, pl.ds(at, 1), :] * e[NH[at * nei + k]]
                        v = t if v is None else v + t
                    store[buf, s] = YB[INTS[sends + at]][:comp] + LH[at][:comp] * v
                start_side(side, after, buf, to[side], both(go, has))

            i = it % ITERS
            if it >= ITERS:
                go_home((0 if ends else 1), 1, i, last)
            elif ends:
                go_home(1, 0, i, last)

            def post(g, _):
                for u in range(8):
                    b = g * 8 + u
                    v = None
                    for k in range(nei):
                        t = F[k, pl.ds(b, 1), :] * e[INTS[k * nb + b]]
                        v = t if v is None else v + t
                    v = YB[b][:comp] + LB[b][:comp] * v
                    XB[b, pl.ds(0, comp), :] = v
                    ahead[b] = v
                return 0

            if sweep < ITERS - 1:
                lax.fori_loop(0, groups, post, 0)
                continue

            def post_level(g, _):
                post(g, 0)
                rows = pl.ds(pl.multiple_of(g * 8, 8), 8)
                acc = None
                for j in range(comp):
                    v = XR[pl.ds(g * 64 + j, 8, stride=8), :]
                    OUT[level, j, rows, :] = v
                    t = v * SH[j, rows, :]
                    acc = t if acc is None else acc + t
                ACC[rows, :] = ACC[rows, :] + W[level] * acc
                return 0

            if not final:
                lax.fori_loop(0, groups, post_level, 0)
            else:
                for i in range(CHUNKS):
                    lax.fori_loop(i * groups // CHUNKS, (i + 1) * groups // CHUNKS, post_level, 0)

                    @pl.when(more)
                    def _():
                        state_copy(i).start()

            if ends:
                for i in range(PIECES):
                    stay(level, i, False)

    def piece(i):
        cut = [j * groups // PIECES * 8 for j in range(PIECES + 1)]
        return pl.ds(cut[i], cut[i + 1] - cut[i])

    def home_copy(slab, level, i):
        out, sem, dev = (OUTA, oas, home_a) if slab else (OUTB, obs, home_b)
        return remote(out.at[level, :, piece(i)], adj_o.at[level, :, piece(i)],
                      sem.at[level, i], ors.at[level, i], dev)

    def here_copy(slab, level, i):
        out, sem = (OUTA, oas) if slab else (OUTB, obs)
        return pltpu.make_async_copy(out.at[level, :, piece(i)], adj_o.at[level, :, piece(i)],
                                     sem.at[level, i])

    def go_home(slab, level, i, cond, wait=False):
        def there():
            copy = home_copy(slab, level, i)
            copy.wait_send() if wait else copy.start()

        def here():
            copy = here_copy(slab, level, i)
            copy.wait() if wait else copy.start()

        if slab:
            pl.when(both(cond, self_a))(here)
            pl.when(both(cond, jnp.logical_not(self_a)))(there)
        else:
            pl.when(cond)(there)

    def stay(level, i, wait):
        @pl.when(native)
        def _():
            copy = here_copy(0, level, i)
            copy.wait() if wait else copy.start()

    def part_copy():
        return remote(PART, RED, pss, psr, nxt)

    def total_copy(t):
        return remote(PART, TOT, fss.at[t], fsr, (t, p))

    @pl.when(active)
    def _():
        zero = jnp.zeros((comp, cells), F32)
        for e in E:
            e[nb + 2 * halo] = zero

            @pl.when(jnp.logical_not(has_lo))
            def _():
                for s in range(halo):
                    e[nb + s] = zero

            @pl.when(jnp.logical_not(has_hi))
            def _():
                for s in range(halo):
                    e[nb + halo + s] = zero

        for g in range(groups):
            ACC[pl.ds(g * 8, 8), :] = jnp.zeros((8, cells), F32)

        @pl.when(native)
        def _():
            for copy in local:
                copy.wait()
            halo_tables()

        @pl.when(onpath)
        def _():
            for copy in coefficients(worker):
                copy.wait_recv()
            copy = pltpu.make_async_copy(IV, INTS, isem)
            copy.start()
            copy.wait()

            @pl.when(self_a)
            def _():
                for copy in self_operands:
                    copy.wait()

            @pl.when(jnp.logical_not(self_a))
            def _():
                for copy in slab_operands(KA, SRCA, WA, ra, worker):
                    copy.wait_recv()

            halo_tables()
            prepare_slab(KA, LPA, LPMA, LBA, LAR, LHA)
            for copy in slab_operands(KB, SRCB, WB, rb, worker):
                copy.wait_recv()

        prepare_slab(KB, LPB, LPMB, LBB, LBR, LHB)

        @pl.when(onpath)
        def _():
            run_slab(KA, SRCA, LPA, LPMA, LBA, LHA, WA, OUTA, False, None)

        run_slab(KB, SRCB, LPB, LPMB, LBB, LHB, WB, OUTB, True, onpath)

        early = both(onpath, jnp.logical_not(last))
        for i in range(PIECES):
            go_home(0, 0, i, onpath)

        PART[...] = jnp.sum(ACC[...].T, axis=0, keepdims=True)

        @pl.when(later)
        def _():
            part_copy().wait_recv()
            PART[...] = PART[...] + RED[...]

        @pl.when(more)
        def _():
            part_copy().start()

        @pl.when(last)
        def _():
            for t in range(n_tm):
                @pl.when(jnp.logical_not(same((t, p))))
                def _():
                    total_copy(t).start()

        for i in range(PIECES):
            go_home(1, 1, i, early)
            go_home(1, 0, i, early)
            go_home(0, 1, i, early)

    @pl.when(both(last, own_summer))
    def _():
        sens_o[...] = PART[...]

    @pl.when(jnp.logical_not(own_summer))
    def _():
        total_copy(0).wait_recv()
        sens_o[...] = TOT[...]

    @pl.when(last)
    def _():
        for t in range(n_tm):
            @pl.when(jnp.logical_not(same((t, p))))
            def _():
                total_copy(t).wait_send()

    @pl.when(more)
    def _():
        for i in range(CHUNKS):
            state_copy(i).wait_send()
        part_copy().wait_send()

    for side, has in ((0, has_lo), (1, has_hi)):
        @pl.when(both(active, has))
        def _():
            halo_copy(side, 0, (SWEEPS - 2) % 2, lo).wait_send()

        @pl.when(both(more, has))
        def _():
            halo_copy(side, 0, (SWEEPS - 1) % 2, lo).wait_send()

    for level in range(STEPS):
        for i in range(PIECES):
            go_home(1, level, i, onpath, True)
            go_home(0, level, i, onpath, True)
            stay(level, i, True)

    @pl.when(both(mover, odd, jnp.logical_not(own_worker)))
    def _():
        for copy in slab_operands(KA, SRCA, WA, ra, worker):
            copy.wait_send()

    @pl.when(both(mover, jnp.logical_not(odd)))
    def _():
        for copy in coefficients(worker):
            copy.wait_send()
        for copy in slab_operands(KB, SRCB, WB, rb, worker):
            copy.wait_send()

    @pl.when(both(mover, jnp.logical_not(own_worker)))
    def _():
        for level in range(STEPS):
            for i in range(PIECES):
                home_copy(0, level, i).wait_recv()


def per_device(source, terminal, jacobian, face_coef, cell_coef, neighbours, send_blocks,
               live_count, volume, shape_field, weights):
    nb, comp, cells = terminal.shape
    nei = face_coef.shape[1]
    halo = send_blocks.shape[2]
    anys = pl.BlockSpec(memory_space=pl.ANY)
    smem = pl.BlockSpec(memory_space=pltpu.SMEM)
    vmem = pltpu.VMEM
    dma = pltpu.SemaphoreType.DMA
    table = nb + 2 * halo + 1
    ints = jnp.concatenate(
        [
            neighbours.T.reshape(nei * nb),
            send_blocks.reshape(2 * halo),
            live_count,
            jnp.zeros(((8 - nei) * nb - 2 * halo - 1,), jnp.int32),
        ]
    )
    slab = vmem((comp, nb, cells), F32)
    plane = vmem((nb, cells), F32)
    rows8 = vmem((nb, 8, cells), F32)
    adj, sens = pl.pallas_call(
        kernel,
        out_shape=(
            jax.ShapeDtypeStruct((STEPS, comp, nb, cells), F32),
            jax.ShapeDtypeStruct((1, nb), F32),
        ),
        in_specs=[anys] * 8 + [smem],
        out_specs=(anys, pl.BlockSpec(memory_space=pltpu.VMEM)),
        scratch_shapes=[
            vmem((comp, comp, nb, cells), F32),
            vmem((comp, comp, nb, cells), F32),
            vmem((STEPS, comp, nb, cells), F32),
            vmem((STEPS, comp, nb, cells), F32),
            vmem((nei, nb, cells), F32),
            plane, plane, plane, plane,
            slab,
            slab, slab, slab, slab,
            rows8, rows8,
            slab, slab,
            rows8, rows8,
            vmem((table, comp, cells), F32),
            vmem((table, comp, cells), F32),
            vmem((table, comp, cells), F32),
            vmem((2, halo, comp, cells), F32),
            vmem((2, halo, comp, cells), F32),
            vmem((STEPS, comp, nb, cells), F32),
            vmem((STEPS, comp, nb, cells), F32),
            plane,
            vmem((1, nb), F32),
            vmem((1, nb), F32),
            vmem((1, nb), F32),
            vmem((STEPS, 1, cells), F32),
            vmem((STEPS, 1, cells), F32),
            vmem((STEPS, 1, cells), F32),
            vmem((8 * nb,), jnp.int32),
            pltpu.SMEM((8 * nb,), jnp.int32),
            vmem((nei, 2 * halo, cells), F32),
            vmem((2 * halo, 8, cells), F32),
            vmem((2 * halo, 8, cells), F32),
            pltpu.SMEM((2 * halo * nei,), jnp.int32),
            dma((3,)),
            dma((3,)),
            dma((3,)),
            dma((5,)),
            dma((5,)),
            dma(()),
            dma((CHUNKS,)),
            dma((SLOTS,)),
            dma((SLOTS,)),
            dma((2,)),
            dma((2,)),
            dma((STEPS, PIECES)),
            dma((STEPS, PIECES)),
            dma((STEPS, PIECES)),
            dma((CHUNKS,)),
            dma(()),
            dma(()),
            dma((lax.axis_size("tm"),)),
            dma(()),
        ],
        compiler_params=pltpu.CompilerParams(collective_id=0, has_side_effects=True),
        name="sweep",
    )(
        source.transpose(0, 2, 1, 3),
        terminal.transpose(1, 0, 2),
        jacobian.transpose(0, 2, 3, 1, 4),
        face_coef.transpose(1, 0, 2),
        cell_coef,
        ints,
        volume,
        shape_field.transpose(1, 0, 2),
        weights,
    )
    return adj.transpose(0, 2, 1, 3), sens.reshape(nb)


def solution(mesh):
    return jax.shard_map(
        per_device,
        mesh=mesh,
        in_specs=(
            P("tm", "space", None, None),
            P("space", None, None),
            P("tm", "space", None, None, None),
            P("space", None, None),
            P("space", None),
            P("space", None),
            P("space", None, None),
            P("space"),
            P("space", None),
            P("space", None, None),
            P("tm"),
        ),
        out_specs=(P("tm", "space", None, None), P("space")),
        check_vma=False,
    )
```

```python
import functools

import jax
import jax.numpy as jnp
from jax import lax
from jax.experimental import pallas as pl
from jax.experimental.pallas import tpu as pltpu
from jax.sharding import PartitionSpec as P

ITERS = 3
STEPS = 2
SWEEPS = ITERS * STEPS
SLOTS = 3
CHUNKS = 4
PIECES = 3
INVERSE_STEP = 6.0
MESH = pl.DeviceIdType.MESH
F32 = jnp.float32


def both(*conds):
    return functools.reduce(jnp.logical_and, conds)


def kernel(
    src_h, term_h, jac_h, face_h, cell_h, ints_h, vol_h, shape_h, w_s,
    adj_o, sens_o,
    KA, KB, SRCA, SRCB, F, CELL, CL, CR, VOL, SH, LPA, LPB, LPMA, LPMB, LBA, LBB,
    R, XIN, XB, YB, E0, E1, E2, SV, SU, SSV, SSU, SF, OUTA, OUTB, ACC, RED, PART, TOT,
    WOUT, WA, WB, IV, INTS, FH, LHA, LHB, NH, NHM, PIV, PINTS, PFH, PLHA, PLHB, PNH,
    ra, rb, sa, rc, sc, vs, vr, vo, go_b, isem, xr, ef, ev, eu, sfs, svs, sus, pps, ppr, oas, obs, ors, hsem, psr, pss, fss, fsr,
):
    comp, nb, cells = XIN.shape
    nei = F.shape[0]
    halo = SF.shape[1]
    groups = nb // 8
    tm = lax.axis_index("tm")
    d = lax.axis_index("space")
    n_tm = lax.axis_size("tm")
    n_sp = lax.axis_size("space")

    x, z, c = tm // 2, d // 4, d % 2
    y = (d // 2) % 2 * 2 + tm % 2

    def path(k, q):
        qz, j = q // 4, q % 4
        qy = jnp.where(qz % 2 == 0, j, 3 - j)
        return 2 * k + qy % 2, 4 * qz + qy // 2 * 2 + 1

    n_planes = n_tm // 2
    native = x == n_planes - 1
    onpath = both(jnp.logical_not(native), c == 1)
    active = jnp.logical_or(native, onpath)
    p = jnp.where(native, d, 4 * z + jnp.where(z % 2 == 0, y, 3 - y))
    first = tm == n_tm - 1
    last = both(onpath, x == 0)
    more = both(active, jnp.logical_not(last))
    later = both(active, jnp.logical_not(first))
    has_lo, has_hi = p > 0, p < n_sp - 1

    def pick(cond, a, b):
        return jnp.where(cond, a[0], b[0]), jnp.where(cond, a[1], b[1])

    def same(dev):
        return both(dev[0] == tm, dev[1] == d)

    def peer(q):
        return pick(native, (tm, q), path(x, q))

    def next_dev(q):
        return pick(first, (tm - 1, q), pick(native, path(x - 1, q), path(jnp.maximum(x - 1, 0), q)))

    def prev_dev(q):
        return pick(native, (tm + 1, q), pick(x == n_planes - 2, (n_tm - 2, q), path(x + 1, q)))

    lo, hi = peer(p - 1), peer(p + 1)
    nxt = next_dev(p)

    up = p % 2 == 1
    slow_q, fast_q = jnp.where(up, p + 1, p - 1), jnp.where(up, p - 1, p + 1)
    has_slow = jnp.where(up, has_hi, has_lo)
    slow, fast = peer(slow_q), peer(fast_q)
    slow_next, fast_next = next_dev(slow_q), next_dev(fast_q)
    slow_off, fast_off = jnp.where(up, halo, 0), jnp.where(up, 0, halo)
    home_a, home_b = (2 * x + 1, p), (2 * x, p)
    self_a = same(home_a)
    mover = jnp.logical_not(native)
    worker = path(x, d)
    own_worker = same(worker)
    odd = tm % 2 == 1

    turned = both(mover, z % 2 == 1)
    via_a, via_b = both(turned, y == 1, c == 0), both(turned, y == 2, c == 1)
    via = jnp.logical_or(via_a, via_b)
    relay_a, relay_b = both(turned, y == 0, c == 0), both(turned, y == 3, c == 0)
    relay = pick(via_a, (2 * x, 4 * z), (2 * x + 1, 4 * z + 2))
    relay_from = pick(relay_a, (2 * x + 1, 4 * z), (2 * x, 4 * z + 3))
    relay_to = path(x, jnp.where(relay_a, 4 * z, 4 * z + 3))
    summer = path(0, d)
    own_summer = same(summer)

    def remote(src, dst, ssem, rsem, dev):
        return pltpu.make_async_remote_copy(src, dst, ssem, rsem, device_id=dev, device_id_type=MESH)

    local = [
        pltpu.make_async_copy(face_h, F, rc.at[0]),
        pltpu.make_async_copy(cell_h, CELL, rc.at[1]),
        pltpu.make_async_copy(vol_h, VOL, rc.at[2]),
        pltpu.make_async_copy(shape_h, SH, rc.at[3]),
        pltpu.make_async_copy(ints_h, INTS, isem),
        pltpu.make_async_copy(jac_h.at[0], KB, rb.at[0]),
        pltpu.make_async_copy(src_h, SRCB, rb.at[1]),
    ]

    @pl.when(native)
    def _():
        for copy in local:
            copy.start()

    term_copy = pltpu.make_async_copy(term_h, XIN, xr.at[0])

    @pl.when(first)
    def _():
        term_copy.start()

    barrier = pltpu.get_barrier_semaphore()
    edges = [(both(active, has_lo), lo), (both(active, has_hi), hi)]
    for ds in (-1, 0, 1):
        inside = both(p + ds >= 0, p + ds < n_sp)
        edges.append((both(more, inside), next_dev(p + ds)))
        edges.append((both(later, inside), prev_dev(p + ds)))
    edges.append((both(mover, jnp.logical_not(own_worker)), worker))
    edges.append((both(onpath, jnp.logical_not(self_a)), home_a))
    edges.append((onpath, home_b))
    relays = jnp.logical_or(relay_a, relay_b)
    edges.append((via, relay))
    edges.append((relays, relay_from))
    edges.append((relays, relay_to))
    edges.append((both(onpath, z % 2 == 1, y == 3), (2 * x, 4 * z)))
    edges.append((both(onpath, z % 2 == 1, y == 0), (2 * x + 1, 4 * z + 2)))
    for t in range(n_tm):
        edges.append((both(last, jnp.logical_not(same((t, p)))), (t, p)))
    edges.append((jnp.logical_not(own_summer), summer))
    expect = 0
    for cond, dev in edges:

        @pl.when(cond)
        def _():
            pl.semaphore_signal(barrier, 1, device_id=dev, device_id_type=MESH)

        expect = expect + jnp.where(cond, 1, 0)

    for level in range(STEPS):
        WOUT[level] = jnp.full((1, cells), w_s[level], F32)

        @pl.when(native)
        def _():
            WB[level] = jnp.full((1, cells), w_s[level], F32)

    E = (E0, E1, E2)
    XR, YR, LAR, LBR = (ref.reshape(ref.shape[0] * 8, cells) for ref in (XB, YB, LBA, LBB))
    lane = lax.broadcasted_iota(jnp.int32, (8, cells), 1)
    sub = lax.broadcasted_iota(jnp.int32, (8, cells), 0)
    sends = nei * nb

    def fast_copy(slot, buf, dev):
        return remote(SF.at[buf], E[slot].at[pl.ds(nb + slow_off, halo)], sfs.at[buf], ef.at[slot], dev)

    def whole_copy(m, dev):
        return remote(SSV.at[pl.ds(0, halo)], SV.at[m], svs, ev.at[m], dev)

    def part_of_copy(m, dev):
        return remote(SSU, SU.at[m], sus, eu.at[m], dev)

    def state_copy(i):
        rows = pl.ds(i * (nb // CHUNKS), nb // CHUNKS)
        return remote(OUTB.at[0, :, rows], XIN.at[:, rows], hsem.at[i], xr.at[i], nxt)

    def sent(at):
        side, s = at // halo, at % halo
        return INTS[sends + (fast_off if side else slow_off) + s]

    def halo_tables():
        for s in range(2 * halo):
            b = sent(s)
            for k in range(nei):
                n = INTS[k * nb + b]
                NH[s * nei + k] = n
                if s < halo:
                    r = n - (nb + slow_off)
                    NHM[s * nei + k] = jnp.where((r >= 0) & (r < halo), nb + 2 * halo, n)
                FH[k, pl.ds(s, 1), :] = F[k, b][None, :]

    def peer_face():
        return remote(FH.at[:, pl.ds(0, halo)], PFH, pps.at[0], ppr.at[0], slow)

    def peer_copy_b():
        return remote(LHB.at[pl.ds(0, halo)], PLHB, pps.at[1], ppr.at[1], slow)

    def peer_copy_a():
        return remote(LHA.at[pl.ds(0, halo)], PLHA, pps.at[2], ppr.at[2], slow)

    def peer_ints(src):
        return remote(src, PIV, pps.at[3], ppr.at[3], slow)

    def peer_tables():
        copy = pltpu.make_async_copy(PIV, PINTS, isem)
        copy.start()
        copy.wait()
        for s in range(halo):
            b = PINTS[sends + fast_off + s]
            for k in range(nei):
                r = PINTS[k * nb + b] - (nb + fast_off)
                PNH[s * nei + k] = jnp.where((r >= 0) & (r < halo), r, halo)

    def prepare_slab(K, LP, LPM, LB, LPR, LH):
        lc = INTS[sends + 2 * halo]

        def prepare(g, _):
            rows = pl.ds(pl.multiple_of(g * 8, 8), 8)
            mass = INVERSE_STEP * VOL[rows, :]
            cell = CELL[rows, :]
            fsum = F[0, rows, :]
            for k in range(1, nei):
                fsum = fsum + F[k, rows, :]
            CR[rows, :] = jnp.where(lane == cells - 1, 0.0, cell)
            CL[rows, :] = jnp.where(lane == 0, 0.0, cell)
            live = jnp.where(sub + g * 8 < lc, 1.0, 0.0)
            for j in range(comp):
                lp = live / (mass + K[j, j, rows, :] + fsum + 2.0 * cell)
                lpm = lp * mass
                LP[j, rows, :] = lp
                LPM[j, rows, :] = lpm
                LPR[pl.ds(g * 64 + j, 8, stride=8), :] = lp
                for i in range(comp):
                    k_ij = -lp * K[i, j, rows, :]
                    if i == j:
                        k_ij = k_ij + (live - lpm)
                    K[i, j, rows, :] = k_ij
            return 0

        lax.fori_loop(0, groups, prepare, 0)
        for s in range(2 * halo):
            LH[s] = LB[sent(s)]

    @pl.when(native)
    def _():
        for copy in local:
            copy.wait()
        halo_tables()
        prepare_slab(KB, LPB, LPMB, LBB, LBR, LHB)

    pl.semaphore_wait(barrier, expect)

    @pl.when(both(native, has_slow))
    def _():
        remote(ints_h, PIV, pps.at[3], ppr.at[3], slow).start()

    def coefficients(dev):
        return [
            remote(ints_h, IV, sc.at[4], rc.at[4], dev),
            remote(face_h, F, sc.at[0], rc.at[0], dev),
            remote(cell_h, CELL, sc.at[1], rc.at[1], dev),
            remote(vol_h, VOL, sc.at[2], rc.at[2], dev),
            remote(shape_h, SH, sc.at[3], rc.at[3], dev),
        ]

    def slab_operands(K, SRC, W, sems, dev):
        return [
            remote(jac_h.at[0], K, sa.at[0], sems.at[0], dev),
            remote(src_h, SRC, sa.at[1], sems.at[1], dev),
            remote(WOUT, W, sa.at[2], sems.at[2], dev),
        ]

    def operand_pieces(source):
        if source:
            refs = [(jac_h.at[0, i], KA.at[i]) for i in range(comp)]
            refs += [(src_h.at[i], SRCA.at[i]) for i in range(STEPS)]
            return [remote(a, b, vs.at[i], vr.at[i], relay) for i, (a, b) in enumerate(refs)]
        out = []
        for K, SRC, sems in ((KA, SRCA, ra), (KB, SRCB, rb)):
            refs = [(KA.at[i], K.at[i], sems.at[0]) for i in range(comp)]
            refs += [(SRCA.at[i], SRC.at[i], sems.at[1]) for i in range(STEPS)]
            out.append([remote(a, b, vo.at[i], sem, relay_to) for i, (a, b, sem) in enumerate(refs)])
        return out

    def send_operands(K, SRC, W, sems, wait):
        copies = slab_operands(K, SRC, W, sems, worker)

        @pl.when(jnp.logical_not(via))
        def _():
            for copy in copies[:2]:
                copy.wait_send() if wait else copy.start()

        @pl.when(via)
        def _():
            for copy in operand_pieces(True):
                copy.wait_send() if wait else copy.start()

        copies[2].wait_send() if wait else copies[2].start()

    self_operands = [
        pltpu.make_async_copy(jac_h.at[0], KA, ra.at[0]),
        pltpu.make_async_copy(src_h, SRCA, ra.at[1]),
    ]

    @pl.when(both(mover, odd, jnp.logical_not(own_worker)))
    def _():
        send_operands(KA, SRCA, WA, ra, False)

    @pl.when(both(mover, odd, own_worker))
    def _():
        for copy in self_operands:
            copy.start()
        WA[...] = WOUT[...]

    @pl.when(both(mover, jnp.logical_not(odd)))
    def _():
        for copy in coefficients(worker):
            copy.start()

    @pl.when(relays)
    def _():
        arriving = operand_pieces(True)
        onward_a, onward_b = operand_pieces(False)
        for i in range(comp + STEPS):
            arriving[i].wait_recv()
            pl.when(relay_a)(onward_a[i].start)
            pl.when(relay_b)(onward_b[i].start)

    def send_even():
        pl.semaphore_wait(go_b, 1)
        send_operands(KB, SRCB, WB, rb, False)

    pl.when(both(mover, jnp.logical_not(odd), c == 0))(send_even)

    def spread(g, _):
        rows = pl.ds(pl.multiple_of(g * 8, 8), 8)
        keep = jnp.where(sub + g * 8 < INTS[sends + 2 * halo], 1.0, 0.0)
        for j in range(comp):
            XR[pl.ds(g * 64 + j, 8, stride=8), :] = keep * XIN[j, rows, :]
        for u in range(8):
            E0[g * 8 + u] = XB[g * 8 + u][:comp]
        return 0

    def start_state():
        term_copy.wait()
        lax.fori_loop(0, groups, spread, 0)
        for s in range(halo):
            SSV[s] = XB[sent(s)][:comp]
            SF[1, s] = XB[sent(halo + s)][:comp]

        @pl.when(has_slow)
        def _():
            whole_copy(0, slow).start()

        fast_copy(0, 1, fast).start()

    def run_slab(K, SRC, LP, LPM, LB, LH, PLH, W, OUT, ends, began):
        for it in range(SWEEPS):
            level = STEPS - 1 - it // ITERS
            sweep = it % ITERS
            slot = it % SLOTS
            buf = it % 2

            def own(g, _):
                rows = pl.ds(pl.multiple_of(g * 8, 8), 8)
                xs = [XR[pl.ds(g * 64 + j, 8, stride=8), :] for j in range(comp)]
                cl, cr = CL[rows, :], CR[rows, :]
                for j in range(comp):
                    lp = LP[j, rows, :]
                    if sweep == 0:
                        v = lp * SRC[level, j, rows, :] + LPM[j, rows, :] * xs[j]
                        R[j, rows, :] = v
                    else:
                        v = R[j, rows, :]
                    for i in range(comp):
                        v = v + K[i, j, rows, :] * xs[i]
                    beside = cl * pltpu.roll(xs[j], 1, 1) + cr * pltpu.roll(xs[j], cells - 1, 1)
                    v = v + lp * beside
                    YR[pl.ds(g * 64 + j, 8, stride=8), :] = v
                return 0

            def spread_own(g, _):
                spread(g, 0)
                own(g, 0)
                return 0

            def arrive():
                for i in range(CHUNKS):
                    state_copy(i).wait_recv()
                    lax.fori_loop(i * groups // CHUNKS, (i + 1) * groups // CHUNKS, spread_own, 0)
                for s in range(halo):
                    SSV[s] = XB[sent(s)][:comp]

            if it == 0 and not ends:
                arrive()
            elif it == 0:
                @pl.when(first)
                def _():
                    start_state()
                    lax.fori_loop(0, groups, own, 0)

                @pl.when(both(native, later))
                def _():
                    arrive()

                @pl.when(onpath)
                def _():
                    lax.fori_loop(0, groups, own, 0)
            else:
                lax.fori_loop(0, groups, own, 0)

            used = None
            if it >= 2:
                used = active
            elif ends:
                used = began if it == 0 else jnp.logical_or(began, first)
            if used is not None:
                @pl.when(used)
                def _():
                    fast_copy(0, buf, fast).wait_send()

                @pl.when(both(used, has_slow))
                def _():
                    (whole_copy(0, slow) if it % 2 else part_of_copy(0, slow)).wait_send()

            e, ahead = E[slot], E[(it + 1) % SLOTS]
            pair = it // 2

            def entry(at, table):
                v = None
                for k in range(nei):
                    t = FH[k, pl.ds(at, 1), :] * e[table[at * nei + k]]
                    v = t if v is None else v + t
                return YB[sent(at)][:comp] + LH[at][:comp] * v

            final = ends and it == SWEEPS - 1
            go = more if final else active
            if it % 2 == 0:
                fast_copy(slot, buf, fast).wait_recv()
                for s in range(halo):
                    SSU[s] = entry(s, NHM)

                @pl.when(has_slow)
                def _():
                    part_of_copy(pair, slow).start()
                    whole_copy(pair, slow).wait_recv()
                    for s in range(halo):
                        e[nb + slow_off + s] = SV[pair, s]
            else:
                if it == 1 and ends:
                    @pl.when(has_slow)
                    def _():
                        peer_copy_b().wait_recv()

                    @pl.when(both(native, has_slow))
                    def _():
                        peer_face().wait_recv()
                        peer_ints(ints_h).wait_recv()
                        peer_tables()

                @pl.when(has_slow)
                def _():
                    part_of_copy(pair, slow).wait_recv()
                    for s in range(halo):
                        v = None
                        for k in range(nei):
                            t = PFH[k, pl.ds(s, 1), :] * SSV[PNH[s * nei + k]]
                            v = t if v is None else v + t
                        e[nb + slow_off + s] = SU[pair, s] + PLH[s][:comp] * v

                fast_copy(slot, buf, fast).wait_recv()
                for s in range(halo):
                    SSV[s] = entry(s, NH)

                @pl.when(both(go, has_slow))
                def _():
                    whole_copy((pair + 1) % 3, slow_next if final else slow).start()

            for s in range(halo):
                SF[buf, s] = entry(halo + s, NH)

            @pl.when(go)
            def _():
                fast_copy((it + 1) % SLOTS, buf, fast_next if final else fast).start()

            i = it % ITERS
            if it >= ITERS:
                go_home((0 if ends else 1), 1, i, last)
            elif ends:
                go_home(1, 0, i, last)

            def post(g, _):
                for u in range(8):
                    b = g * 8 + u
                    v = None
                    for k in range(nei):
                        t = F[k, pl.ds(b, 1), :] * e[INTS[k * nb + b]]
                        v = t if v is None else v + t
                    v = YB[b][:comp] + LB[b][:comp] * v
                    XB[b, pl.ds(0, comp), :] = v
                    ahead[b] = v
                return 0

            if sweep < ITERS - 1:
                lax.fori_loop(0, groups, post, 0)
                continue

            def post_level(g, _):
                post(g, 0)
                rows = pl.ds(pl.multiple_of(g * 8, 8), 8)
                acc = None
                for j in range(comp):
                    v = XR[pl.ds(g * 64 + j, 8, stride=8), :]
                    OUT[level, j, rows, :] = v
                    t = v * SH[j, rows, :]
                    acc = t if acc is None else acc + t
                ACC[rows, :] = ACC[rows, :] + W[level] * acc
                return 0

            if not final:
                lax.fori_loop(0, groups, post_level, 0)
            else:
                for i in range(CHUNKS):
                    lax.fori_loop(i * groups // CHUNKS, (i + 1) * groups // CHUNKS, post_level, 0)

                    @pl.when(more)
                    def _():
                        state_copy(i).start()

            if ends:
                for i in range(PIECES):
                    stay(level, i, False)

    def piece(i):
        cut = [j * groups // PIECES * 8 for j in range(PIECES + 1)]
        return pl.ds(cut[i], cut[i + 1] - cut[i])

    def home_copy(slab, level, i):
        out, sem, dev = (OUTA, oas, home_a) if slab else (OUTB, obs, home_b)
        return remote(out.at[level, :, piece(i)], adj_o.at[level, :, piece(i)],
                      sem.at[level, i], ors.at[level, i], dev)

    def here_copy(slab, level, i):
        out, sem = (OUTA, oas) if slab else (OUTB, obs)
        return pltpu.make_async_copy(out.at[level, :, piece(i)], adj_o.at[level, :, piece(i)],
                                     sem.at[level, i])

    def go_home(slab, level, i, cond, wait=False):
        def there():
            copy = home_copy(slab, level, i)
            copy.wait_send() if wait else copy.start()

        def here():
            copy = here_copy(slab, level, i)
            copy.wait() if wait else copy.start()

        if slab:
            pl.when(both(cond, self_a))(here)
            pl.when(both(cond, jnp.logical_not(self_a)))(there)
        else:
            pl.when(cond)(there)

    def stay(level, i, wait):
        @pl.when(native)
        def _():
            copy = here_copy(0, level, i)
            copy.wait() if wait else copy.start()

    def part_copy():
        return remote(PART, RED, pss, psr, nxt)

    def total_copy(t):
        return remote(PART, TOT, fss.at[t], fsr, (t, p))

    @pl.when(active)
    def _():
        zero = jnp.zeros((comp, cells), F32)
        for e in E:
            e[nb + 2 * halo] = zero

            @pl.when(jnp.logical_not(has_slow))
            def _():
                for s in range(halo):
                    e[nb + slow_off + s] = zero

        SSV[halo] = zero
        for g in range(groups):
            ACC[pl.ds(g * 8, 8), :] = jnp.zeros((8, cells), F32)

        @pl.when(onpath)
        def _():
            for copy in coefficients(worker):
                copy.wait_recv()
            copy = pltpu.make_async_copy(IV, INTS, isem)
            copy.start()
            copy.wait()

            @pl.when(has_slow)
            def _():
                peer_ints(IV).start()

            @pl.when(self_a)
            def _():
                for copy in self_operands:
                    copy.wait()

            @pl.when(jnp.logical_not(self_a))
            def _():
                for copy in slab_operands(KA, SRCA, WA, ra, worker):
                    copy.wait_recv()

            pl.semaphore_signal(go_b, 1, device_id=home_b, device_id_type=MESH)
            pl.when(jnp.logical_not(odd))(send_even)
            halo_tables()
            prepare_slab(KA, LPA, LPMA, LBA, LAR, LHA)

            @pl.when(has_slow)
            def _():
                peer_face().start()
                peer_copy_a().start()
                for copy in (peer_ints(IV), peer_face(), peer_copy_a()):
                    copy.wait_recv()
                peer_tables()

        def take_b():
            for copy in slab_operands(KB, SRCB, WB, rb, worker):
                copy.wait_recv()
            prepare_slab(KB, LPB, LPMB, LBB, LBR, LHB)

            @pl.when(has_slow)
            def _():
                peer_copy_b().start()

        rushed = x == n_planes - 2
        pl.when(both(onpath, jnp.logical_not(rushed)))(take_b)

        @pl.when(both(native, has_slow))
        def _():
            peer_face().start()
            peer_copy_b().start()

        @pl.when(onpath)
        def _():
            run_slab(KA, SRCA, LPA, LPMA, LBA, LHA, PLHA, WA, OUTA, False, None)
            pl.when(rushed)(take_b)

        run_slab(KB, SRCB, LPB, LPMB, LBB, LHB, PLHB, WB, OUTB, True, onpath)

        early = both(onpath, jnp.logical_not(last))
        for i in range(PIECES):
            go_home(0, 0, i, onpath)

        PART[...] = jnp.sum(ACC[...].T, axis=0, keepdims=True)

        @pl.when(later)
        def _():
            part_copy().wait_recv()
            PART[...] = PART[...] + RED[...]

        @pl.when(more)
        def _():
            part_copy().start()

        @pl.when(last)
        def _():
            for t in range(n_tm):
                @pl.when(jnp.logical_not(same((t, p))))
                def _():
                    total_copy(t).start()

        for i in range(PIECES):
            go_home(1, 1, i, early)
            go_home(1, 0, i, early)
            go_home(0, 1, i, early)

    @pl.when(both(last, own_summer))
    def _():
        sens_o[...] = PART[...]

    @pl.when(jnp.logical_not(own_summer))
    def _():
        total_copy(0).wait_recv()
        sens_o[...] = TOT[...]

    @pl.when(last)
    def _():
        for t in range(n_tm):
            @pl.when(jnp.logical_not(same((t, p))))
            def _():
                total_copy(t).wait_send()

    @pl.when(more)
    def _():
        for i in range(CHUNKS):
            state_copy(i).wait_send()
        part_copy().wait_send()

    @pl.when(active)
    def _():
        fast_copy(0, (SWEEPS - 2) % 2, fast).wait_send()

    @pl.when(more)
    def _():
        fast_copy(0, (SWEEPS - 1) % 2, fast).wait_send()

    @pl.when(both(active, has_slow))
    def _():
        part_of_copy(0, slow).wait_send()
        peer_ints(IV).wait_send()
        peer_face().wait_send()
        peer_copy_b().wait_send()

    @pl.when(both(onpath, has_slow))
    def _():
        peer_copy_a().wait_send()

    @pl.when(both(more, has_slow))
    def _():
        whole_copy(0, slow).wait_send()

    for level in range(STEPS):
        for i in range(PIECES):
            go_home(1, level, i, onpath, True)
            go_home(0, level, i, onpath, True)
            stay(level, i, True)

    @pl.when(both(mover, odd, jnp.logical_not(own_worker)))
    def _():
        send_operands(KA, SRCA, WA, ra, True)

    @pl.when(both(mover, jnp.logical_not(odd)))
    def _():
        for copy in coefficients(worker):
            copy.wait_send()
        send_operands(KB, SRCB, WB, rb, True)

    @pl.when(relays)
    def _():
        onward_a, onward_b = operand_pieces(False)
        for i in range(comp + STEPS):
            pl.when(relay_a)(onward_a[i].wait_send)
            pl.when(relay_b)(onward_b[i].wait_send)

    @pl.when(both(mover, jnp.logical_not(own_worker)))
    def _():
        for level in range(STEPS):
            for i in range(PIECES):
                home_copy(0, level, i).wait_recv()


def per_device(source, terminal, jacobian, face_coef, cell_coef, neighbours, send_blocks,
               live_count, volume, shape_field, weights):
    nb, comp, cells = terminal.shape
    nei = face_coef.shape[1]
    halo = send_blocks.shape[2]
    anys = pl.BlockSpec(memory_space=pl.ANY)
    smem = pl.BlockSpec(memory_space=pltpu.SMEM)
    vmem = pltpu.VMEM
    dma = pltpu.SemaphoreType.DMA
    table = nb + 2 * halo + 1
    ints = jnp.concatenate(
        [
            neighbours.T.reshape(nei * nb),
            send_blocks.reshape(2 * halo),
            live_count,
            jnp.zeros(((8 - nei) * nb - 2 * halo - 1,), jnp.int32),
        ]
    )
    slab = vmem((comp, nb, cells), F32)
    plane = vmem((nb, cells), F32)
    rows8 = vmem((nb, 8, cells), F32)
    adj, sens = pl.pallas_call(
        kernel,
        out_shape=(
            jax.ShapeDtypeStruct((STEPS, comp, nb, cells), F32),
            jax.ShapeDtypeStruct((1, nb), F32),
        ),
        in_specs=[anys] * 8 + [smem],
        out_specs=(anys, pl.BlockSpec(memory_space=pltpu.VMEM)),
        scratch_shapes=[
            vmem((comp, comp, nb, cells), F32),
            vmem((comp, comp, nb, cells), F32),
            vmem((STEPS, comp, nb, cells), F32),
            vmem((STEPS, comp, nb, cells), F32),
            vmem((nei, nb, cells), F32),
            plane, plane, plane, plane,
            slab,
            slab, slab, slab, slab,
            rows8, rows8,
            slab, slab,
            rows8, rows8,
            vmem((table, comp, cells), F32),
            vmem((table, comp, cells), F32),
            vmem((table, comp, cells), F32),
            vmem((3, halo, comp, cells), F32),
            vmem((3, halo, comp, cells), F32),
            vmem((halo + 1, comp, cells), F32),
            vmem((halo, comp, cells), F32),
            vmem((2, halo, comp, cells), F32),
            vmem((STEPS, comp, nb, cells), F32),
            vmem((STEPS, comp, nb, cells), F32),
            plane,
            vmem((1, nb), F32),
            vmem((1, nb), F32),
            vmem((1, nb), F32),
            vmem((STEPS, 1, cells), F32),
            vmem((STEPS, 1, cells), F32),
            vmem((STEPS, 1, cells), F32),
            vmem((8 * nb,), jnp.int32),
            pltpu.SMEM((8 * nb,), jnp.int32),
            vmem((nei, 2 * halo, cells), F32),
            vmem((2 * halo, 8, cells), F32),
            vmem((2 * halo, 8, cells), F32),
            pltpu.SMEM((2 * halo * nei,), jnp.int32),
            pltpu.SMEM((halo * nei,), jnp.int32),
            vmem((8 * nb,), jnp.int32),
            pltpu.SMEM((8 * nb,), jnp.int32),
            vmem((nei, halo, cells), F32),
            vmem((halo, 8, cells), F32),
            vmem((halo, 8, cells), F32),
            pltpu.SMEM((halo * nei,), jnp.int32),
            dma((3,)),
            dma((3,)),
            dma((3,)),
            dma((5,)),
            dma((5,)),
            dma((comp + STEPS,)),
            dma((comp + STEPS,)),
            dma((comp + STEPS,)),
            pltpu.SemaphoreType.REGULAR,
            dma(()),
            dma((CHUNKS,)),
            dma((SLOTS,)),
            dma((3,)),
            dma((3,)),
            dma((2,)),
            dma(()),
            dma(()),
            dma((4,)),
            dma((4,)),
            dma((STEPS, PIECES)),
            dma((STEPS, PIECES)),
            dma((STEPS, PIECES)),
            dma((CHUNKS,)),
            dma(()),
            dma(()),
            dma((lax.axis_size("tm"),)),
            dma(()),
        ],
        compiler_params=pltpu.CompilerParams(collective_id=0, has_side_effects=True),
        name="sweep",
    )(
        source.transpose(0, 2, 1, 3),
        terminal.transpose(1, 0, 2),
        jacobian.transpose(0, 2, 3, 1, 4),
        face_coef.transpose(1, 0, 2),
        cell_coef,
        ints,
        volume,
        shape_field.transpose(1, 0, 2),
        weights,
    )
    return adj.transpose(0, 2, 1, 3), sens.reshape(nb)


def solution(mesh):
    return jax.shard_map(
        per_device,
        mesh=mesh,
        in_specs=(
            P("tm", "space", None, None),
            P("space", None, None),
            P("tm", "space", None, None, None),
            P("space", None, None),
            P("space", None),
            P("space", None),
            P("space", None, None),
            P("space"),
            P("space", None),
            P("space", None, None),
            P("tm"),
        ),
        out_specs=(P("tm", "space", None, None), P("space")),
        check_vma=False,
    )
```

```python
import functools

import jax
import jax.numpy as jnp
from jax import lax
from jax.experimental import pallas as pl
from jax.experimental.pallas import tpu as pltpu
from jax.sharding import PartitionSpec as P

ITERS = 3
STEPS = 2
SWEEPS = ITERS * STEPS
SLOTS = 3
CHUNKS = 8
PIECES = 3
INVERSE_STEP = 6.0
MESH = pl.DeviceIdType.MESH
F32 = jnp.float32


def both(*conds):
    return functools.reduce(jnp.logical_and, conds)


def kernel(
    src_h, term_h, jac_h, face_h, cell_h, ints_h, vol_h, shape_h, w_s,
    adj_o, sens_o,
    KA, KB, SRCA, SRCB, F, CELL, CL, CR, VOL, SH, LPA, LPB, LPMA, LPMB, LBA, LBB,
    R, XIN, XB, YB, E0, E1, E2, SV, SU, SSV, SSU, SF, OUTA, OUTB, ACC, RED, PART, TOT,
    WOUT, WA, WB, IV, INTS, FH, LHA, LHB, NH, NHM, PIV, PINTS, PFH, PLHA, PLHB, PNH,
    ra, rb, sa, rc, sc, vs, vr, vo, go_b, isem, xr, ef, ev, eu, sfs, svs, sus, pps, ppr, oas, obs, ors, hsem, psr, pss, fss, fsr,
):
    comp, nb, cells = XIN.shape
    nei = F.shape[0]
    halo = SF.shape[1]
    groups = nb // 8
    tm = lax.axis_index("tm")
    d = lax.axis_index("space")
    n_tm = lax.axis_size("tm")
    n_sp = lax.axis_size("space")

    x, z, c = tm // 2, d // 4, d % 2
    y = (d // 2) % 2 * 2 + tm % 2

    def path(k, q):
        qz, j = q // 4, q % 4
        qy = jnp.where(qz % 2 == 0, j, 3 - j)
        return 2 * k + qy % 2, 4 * qz + qy // 2 * 2 + 1

    n_planes = n_tm // 2
    native = x == n_planes - 1
    onpath = both(jnp.logical_not(native), c == 1)
    active = jnp.logical_or(native, onpath)
    p = jnp.where(native, d, 4 * z + jnp.where(z % 2 == 0, y, 3 - y))
    first = tm == n_tm - 1
    last = both(onpath, x == 0)
    more = both(active, jnp.logical_not(last))
    later = both(active, jnp.logical_not(first))
    has_lo, has_hi = p > 0, p < n_sp - 1

    def pick(cond, a, b):
        return jnp.where(cond, a[0], b[0]), jnp.where(cond, a[1], b[1])

    def same(dev):
        return both(dev[0] == tm, dev[1] == d)

    def peer(q):
        return pick(native, (tm, q), path(x, q))

    def next_dev(q):
        return pick(first, (tm - 1, q), pick(native, path(x - 1, q), path(jnp.maximum(x - 1, 0), q)))

    def prev_dev(q):
        return pick(native, (tm + 1, q), pick(x == n_planes - 2, (n_tm - 2, q), path(x + 1, q)))

    lo, hi = peer(p - 1), peer(p + 1)
    nxt = next_dev(p)

    up = p % 2 == 1
    slow_q, fast_q = jnp.where(up, p + 1, p - 1), jnp.where(up, p - 1, p + 1)
    has_slow = jnp.where(up, has_hi, has_lo)
    slow, fast = peer(slow_q), peer(fast_q)
    slow_next, fast_next = next_dev(slow_q), next_dev(fast_q)
    slow_off, fast_off = jnp.where(up, halo, 0), jnp.where(up, 0, halo)
    home_a, home_b = (2 * x + 1, p), (2 * x, p)
    self_a = same(home_a)
    mover = jnp.logical_not(native)
    worker = path(x, d)
    own_worker = same(worker)
    odd = tm % 2 == 1

    turned = both(mover, z % 2 == 1)
    via_a, via_b = both(turned, y == 1, c == 0), both(turned, y == 2, c == 1)
    via = jnp.logical_or(via_a, via_b)
    relay_a, relay_b = both(turned, y == 0, c == 0), both(turned, y == 3, c == 0)
    relay = pick(via_a, (2 * x, 4 * z), (2 * x + 1, 4 * z + 2))
    relay_from = pick(relay_a, (2 * x + 1, 4 * z), (2 * x, 4 * z + 3))
    relay_to = path(x, jnp.where(relay_a, 4 * z, 4 * z + 3))
    summer = path(0, d)
    own_summer = same(summer)

    def remote(src, dst, ssem, rsem, dev):
        return pltpu.make_async_remote_copy(src, dst, ssem, rsem, device_id=dev, device_id_type=MESH)

    local = [
        pltpu.make_async_copy(face_h, F, rc.at[0]),
        pltpu.make_async_copy(cell_h, CELL, rc.at[1]),
        pltpu.make_async_copy(vol_h, VOL, rc.at[2]),
        pltpu.make_async_copy(shape_h, SH, rc.at[3]),
        pltpu.make_async_copy(ints_h, INTS, isem),
        pltpu.make_async_copy(jac_h.at[0], KB, rb.at[0]),
        pltpu.make_async_copy(src_h, SRCB, rb.at[1]),
    ]

    @pl.when(native)
    def _():
        for copy in local:
            copy.start()

    term_copy = pltpu.make_async_copy(term_h, XIN, xr.at[0])

    @pl.when(first)
    def _():
        term_copy.start()

    barrier = pltpu.get_barrier_semaphore()
    edges = [(both(active, has_lo), lo), (both(active, has_hi), hi)]
    for ds in (-1, 0, 1):
        inside = both(p + ds >= 0, p + ds < n_sp)
        edges.append((both(more, inside), next_dev(p + ds)))
        edges.append((both(later, inside), prev_dev(p + ds)))
    edges.append((both(mover, jnp.logical_not(own_worker)), worker))
    edges.append((both(onpath, jnp.logical_not(self_a)), home_a))
    edges.append((onpath, home_b))
    relays = jnp.logical_or(relay_a, relay_b)
    edges.append((via, relay))
    edges.append((relays, relay_from))
    edges.append((relays, relay_to))
    edges.append((both(onpath, z % 2 == 1, y == 3), (2 * x, 4 * z)))
    edges.append((both(onpath, z % 2 == 1, y == 0), (2 * x + 1, 4 * z + 2)))
    for t in range(n_tm):
        edges.append((both(last, jnp.logical_not(same((t, p)))), (t, p)))
    edges.append((jnp.logical_not(own_summer), summer))
    expect = 0
    for cond, dev in edges:

        @pl.when(cond)
        def _():
            pl.semaphore_signal(barrier, 1, device_id=dev, device_id_type=MESH)

        expect = expect + jnp.where(cond, 1, 0)

    for level in range(STEPS):
        WOUT[level] = jnp.full((1, cells), w_s[level], F32)

        @pl.when(native)
        def _():
            WB[level] = jnp.full((1, cells), w_s[level], F32)

    E = (E0, E1, E2)
    XR, YR, LAR, LBR = (ref.reshape(ref.shape[0] * 8, cells) for ref in (XB, YB, LBA, LBB))
    lane = lax.broadcasted_iota(jnp.int32, (8, cells), 1)
    sub = lax.broadcasted_iota(jnp.int32, (8, cells), 0)
    sends = nei * nb

    def fast_copy(slot, buf, dev):
        return remote(SF.at[buf], E[slot].at[pl.ds(nb + slow_off, halo)], sfs.at[buf], ef.at[slot], dev)

    def whole_copy(m, dev):
        return remote(SSV.at[pl.ds(0, halo)], SV.at[m], svs, ev.at[m], dev)

    def part_of_copy(m, dev):
        return remote(SSU, SU.at[m], sus, eu.at[m], dev)

    def state_copy(i):
        rows = pl.ds(i * (nb // CHUNKS), nb // CHUNKS)
        return remote(OUTB.at[0, :, rows], XIN.at[:, rows], hsem.at[i], xr.at[i], nxt)

    def sent(at):
        side, s = at // halo, at % halo
        return INTS[sends + (fast_off if side else slow_off) + s]

    def halo_tables():
        for s in range(2 * halo):
            b = sent(s)
            for k in range(nei):
                n = INTS[k * nb + b]
                NH[s * nei + k] = n
                if s < halo:
                    r = n - (nb + slow_off)
                    NHM[s * nei + k] = jnp.where((r >= 0) & (r < halo), nb + 2 * halo, n)
                FH[k, pl.ds(s, 1), :] = F[k, b][None, :]

    def peer_face():
        return remote(FH.at[:, pl.ds(0, halo)], PFH, pps.at[0], ppr.at[0], slow)

    def peer_copy_b():
        return remote(LHB.at[pl.ds(0, halo)], PLHB, pps.at[1], ppr.at[1], slow)

    def peer_copy_a():
        return remote(LHA.at[pl.ds(0, halo)], PLHA, pps.at[2], ppr.at[2], slow)

    def peer_ints(src):
        return remote(src, PIV, pps.at[3], ppr.at[3], slow)

    def peer_tables():
        copy = pltpu.make_async_copy(PIV, PINTS, isem)
        copy.start()
        copy.wait()
        for s in range(halo):
            b = PINTS[sends + fast_off + s]
            for k in range(nei):
                r = PINTS[k * nb + b] - (nb + fast_off)
                PNH[s * nei + k] = jnp.where((r >= 0) & (r < halo), r, halo)

    def prepare_slab(K, LP, LPM, LB, LPR, LH):
        lc = INTS[sends + 2 * halo]

        def prepare(g, _):
            rows = pl.ds(pl.multiple_of(g * 8, 8), 8)
            mass = INVERSE_STEP * VOL[rows, :]
            cell = CELL[rows, :]
            fsum = F[0, rows, :]
            for k in range(1, nei):
                fsum = fsum + F[k, rows, :]
            CR[rows, :] = jnp.where(lane == cells - 1, 0.0, cell)
            CL[rows, :] = jnp.where(lane == 0, 0.0, cell)
            live = jnp.where(sub + g * 8 < lc, 1.0, 0.0)
            for j in range(comp):
                lp = live / (mass + K[j, j, rows, :] + fsum + 2.0 * cell)
                lpm = lp * mass
                LP[j, rows, :] = lp
                LPM[j, rows, :] = lpm
                LPR[pl.ds(g * 64 + j, 8, stride=8), :] = lp
                for i in range(comp):
                    k_ij = -lp * K[i, j, rows, :]
                    if i == j:
                        k_ij = k_ij + (live - lpm)
                    K[i, j, rows, :] = k_ij
            return 0

        lax.fori_loop(0, groups, prepare, 0)
        for s in range(2 * halo):
            LH[s] = LB[sent(s)]

    @pl.when(native)
    def _():
        for copy in local:
            copy.wait()
        halo_tables()
        prepare_slab(KB, LPB, LPMB, LBB, LBR, LHB)

    pl.semaphore_wait(barrier, expect)

    @pl.when(both(native, has_slow))
    def _():
        remote(ints_h, PIV, pps.at[3], ppr.at[3], slow).start()

    def coefficients(dev):
        return [
            remote(ints_h, IV, sc.at[4], rc.at[4], dev),
            remote(face_h, F, sc.at[0], rc.at[0], dev),
            remote(cell_h, CELL, sc.at[1], rc.at[1], dev),
            remote(vol_h, VOL, sc.at[2], rc.at[2], dev),
            remote(shape_h, SH, sc.at[3], rc.at[3], dev),
        ]

    def slab_operands(K, SRC, W, sems, dev):
        return [
            remote(jac_h.at[0], K, sa.at[0], sems.at[0], dev),
            remote(src_h, SRC, sa.at[1], sems.at[1], dev),
            remote(WOUT, W, sa.at[2], sems.at[2], dev),
        ]

    def operand_pieces(source):
        if source:
            refs = [(jac_h.at[0, i], KA.at[i]) for i in range(comp)]
            refs += [(src_h.at[i], SRCA.at[i]) for i in range(STEPS)]
            return [remote(a, b, vs.at[i], vr.at[i], relay) for i, (a, b) in enumerate(refs)]
        out = []
        for K, SRC, sems in ((KA, SRCA, ra), (KB, SRCB, rb)):
            refs = [(KA.at[i], K.at[i], sems.at[0]) for i in range(comp)]
            refs += [(SRCA.at[i], SRC.at[i], sems.at[1]) for i in range(STEPS)]
            out.append([remote(a, b, vo.at[i], sem, relay_to) for i, (a, b, sem) in enumerate(refs)])
        return out

    def send_operands(K, SRC, W, sems, wait):
        copies = slab_operands(K, SRC, W, sems, worker)

        @pl.when(jnp.logical_not(via))
        def _():
            for copy in copies[:2]:
                copy.wait_send() if wait else copy.start()

        @pl.when(via)
        def _():
            for copy in operand_pieces(True):
                copy.wait_send() if wait else copy.start()

        copies[2].wait_send() if wait else copies[2].start()

    self_operands = [
        pltpu.make_async_copy(jac_h.at[0], KA, ra.at[0]),
        pltpu.make_async_copy(src_h, SRCA, ra.at[1]),
    ]

    @pl.when(both(mover, odd, jnp.logical_not(own_worker)))
    def _():
        send_operands(KA, SRCA, WA, ra, False)

    @pl.when(both(mover, odd, own_worker))
    def _():
        for copy in self_operands:
            copy.start()
        WA[...] = WOUT[...]

    @pl.when(both(mover, jnp.logical_not(odd)))
    def _():
        for copy in coefficients(worker):
            copy.start()

    @pl.when(relays)
    def _():
        arriving = operand_pieces(True)
        onward_a, onward_b = operand_pieces(False)
        for i in range(comp + STEPS):
            arriving[i].wait_recv()
            pl.when(relay_a)(onward_a[i].start)
            pl.when(relay_b)(onward_b[i].start)

    def send_even():
        pl.semaphore_wait(go_b, 1)
        send_operands(KB, SRCB, WB, rb, False)

    pl.when(both(mover, jnp.logical_not(odd), c == 0))(send_even)

    def spread(g, _):
        rows = pl.ds(pl.multiple_of(g * 8, 8), 8)
        keep = jnp.where(sub + g * 8 < INTS[sends + 2 * halo], 1.0, 0.0)
        for j in range(comp):
            XR[pl.ds(g * 64 + j, 8, stride=8), :] = keep * XIN[j, rows, :]
        for u in range(8):
            E0[g * 8 + u] = XB[g * 8 + u][:comp]
        return 0

    def start_state():
        term_copy.wait()
        lax.fori_loop(0, groups, spread, 0)
        for s in range(halo):
            SSV[s] = XB[sent(s)][:comp]
            SF[1, s] = XB[sent(halo + s)][:comp]

        @pl.when(has_slow)
        def _():
            whole_copy(0, slow).start()

        fast_copy(0, 1, fast).start()

    def run_slab(K, SRC, LP, LPM, LB, LH, PLH, W, OUT, ends, began):
        for it in range(SWEEPS):
            level = STEPS - 1 - it // ITERS
            sweep = it % ITERS
            slot = it % SLOTS
            buf = it % 2

            def own(g, _):
                rows = pl.ds(pl.multiple_of(g * 8, 8), 8)
                xs = [XR[pl.ds(g * 64 + j, 8, stride=8), :] for j in range(comp)]
                cl, cr = CL[rows, :], CR[rows, :]
                for j in range(comp):
                    lp = LP[j, rows, :]
                    if sweep == 0:
                        v = lp * SRC[level, j, rows, :] + LPM[j, rows, :] * xs[j]
                        R[j, rows, :] = v
                    else:
                        v = R[j, rows, :]
                    for i in range(comp):
                        v = v + K[i, j, rows, :] * xs[i]
                    beside = cl * pltpu.roll(xs[j], 1, 1) + cr * pltpu.roll(xs[j], cells - 1, 1)
                    v = v + lp * beside
                    YR[pl.ds(g * 64 + j, 8, stride=8), :] = v
                return 0

            def spread_own(g, _):
                spread(g, 0)
                own(g, 0)
                return 0

            def arrive():
                for i in range(CHUNKS):
                    state_copy(i).wait_recv()
                    lax.fori_loop(i * groups // CHUNKS, (i + 1) * groups // CHUNKS, spread_own, 0)
                for s in range(halo):
                    SSV[s] = XB[sent(s)][:comp]

            if it == 0 and not ends:
                arrive()
            elif it == 0:
                @pl.when(first)
                def _():
                    start_state()
                    lax.fori_loop(0, groups, own, 0)

                @pl.when(both(native, later))
                def _():
                    arrive()

                @pl.when(onpath)
                def _():
                    lax.fori_loop(0, groups, own, 0)
            else:
                lax.fori_loop(0, groups, own, 0)

            used = None
            if it >= 2:
                used = active
            elif ends:
                used = began if it == 0 else jnp.logical_or(began, first)
            if used is not None:
                @pl.when(used)
                def _():
                    fast_copy(0, buf, fast).wait_send()

                @pl.when(both(used, has_slow))
                def _():
                    (whole_copy(0, slow) if it % 2 else part_of_copy(0, slow)).wait_send()

            e, ahead = E[slot], E[(it + 1) % SLOTS]
            pair = it // 2

            def entry(at, table):
                v = None
                for k in range(nei):
                    t = FH[k, pl.ds(at, 1), :] * e[table[at * nei + k]]
                    v = t if v is None else v + t
                return YB[sent(at)][:comp] + LH[at][:comp] * v

            final = ends and it == SWEEPS - 1
            go = more if final else active

            def taken(f):
                pl.when(more)(f) if final else f()
            if it % 2 == 0:
                fast_copy(slot, buf, fast).wait_recv()
                for s in range(halo):
                    SSU[s] = entry(s, NHM)

                @pl.when(has_slow)
                def _():
                    part_of_copy(pair, slow).start()
                    whole_copy(pair, slow).wait_recv()
                    for s in range(halo):
                        e[nb + slow_off + s] = SV[pair, s]
            else:
                if it == 1 and ends:
                    @pl.when(has_slow)
                    def _():
                        peer_copy_b().wait_recv()

                    @pl.when(both(native, has_slow))
                    def _():
                        peer_face().wait_recv()
                        peer_ints(ints_h).wait_recv()
                        peer_tables()

                @pl.when(has_slow)
                def _():
                    part_of_copy(pair, slow).wait_recv()
                    for s in range(halo):
                        v = None
                        for k in range(nei):
                            t = PFH[k, pl.ds(s, 1), :] * SSV[PNH[s * nei + k]]
                            v = t if v is None else v + t
                        e[nb + slow_off + s] = SU[pair, s] + PLH[s][:comp] * v

                fast_copy(slot, buf, fast).wait_recv()
                def whole():
                    for s in range(halo):
                        SSV[s] = entry(s, NH)

                taken(whole)

                @pl.when(both(go, has_slow))
                def _():
                    whole_copy((pair + 1) % 3, slow_next if final else slow).start()

            def quick():
                for s in range(halo):
                    SF[buf, s] = entry(halo + s, NH)

            taken(quick)

            @pl.when(go)
            def _():
                fast_copy((it + 1) % SLOTS, buf, fast_next if final else fast).start()

            i = it % ITERS
            if it >= ITERS:
                go_home((0 if ends else 1), 1, i, last)
            elif ends:
                go_home(1, 0, i, last)

            def post(g, _):
                for u in range(8):
                    b = g * 8 + u
                    v = None
                    for k in range(nei):
                        t = F[k, pl.ds(b, 1), :] * e[INTS[k * nb + b]]
                        v = t if v is None else v + t
                    v = YB[b][:comp] + LB[b][:comp] * v
                    XB[b, pl.ds(0, comp), :] = v
                    ahead[b] = v
                return 0

            if sweep < ITERS - 1:
                lax.fori_loop(0, groups, post, 0)
                continue

            def post_level(g, _):
                post(g, 0)
                rows = pl.ds(pl.multiple_of(g * 8, 8), 8)
                acc = None
                for j in range(comp):
                    v = XR[pl.ds(g * 64 + j, 8, stride=8), :]
                    OUT[level, j, rows, :] = v
                    t = v * SH[j, rows, :]
                    acc = t if acc is None else acc + t
                ACC[rows, :] = ACC[rows, :] + W[level] * acc
                return 0

            if not final:
                lax.fori_loop(0, groups, post_level, 0)
            else:
                for i in range(CHUNKS):
                    lax.fori_loop(i * groups // CHUNKS, (i + 1) * groups // CHUNKS, post_level, 0)

                    @pl.when(more)
                    def _():
                        state_copy(i).start()

                    for j in range(PIECES):
                        if i * groups // CHUNKS < (j + 1) * groups // PIECES <= (i + 1) * groups // CHUNKS:
                            go_home(0, 0, j, last)

            if ends:
                for i in range(PIECES):
                    stay(level, i, False)

    def piece(i):
        cut = [j * groups // PIECES * 8 for j in range(PIECES + 1)]
        return pl.ds(cut[i], cut[i + 1] - cut[i])

    def home_copy(slab, level, i):
        out, sem, dev = (OUTA, oas, home_a) if slab else (OUTB, obs, home_b)
        return remote(out.at[level, :, piece(i)], adj_o.at[level, :, piece(i)],
                      sem.at[level, i], ors.at[level, i], dev)

    def here_copy(slab, level, i):
        out, sem = (OUTA, oas) if slab else (OUTB, obs)
        return pltpu.make_async_copy(out.at[level, :, piece(i)], adj_o.at[level, :, piece(i)],
                                     sem.at[level, i])

    def go_home(slab, level, i, cond, wait=False):
        def there():
            copy = home_copy(slab, level, i)
            copy.wait_send() if wait else copy.start()

        def here():
            copy = here_copy(slab, level, i)
            copy.wait() if wait else copy.start()

        if slab:
            pl.when(both(cond, self_a))(here)
            pl.when(both(cond, jnp.logical_not(self_a)))(there)
        else:
            pl.when(cond)(there)

    def stay(level, i, wait):
        @pl.when(native)
        def _():
            copy = here_copy(0, level, i)
            copy.wait() if wait else copy.start()

    def part_copy():
        return remote(PART, RED, pss, psr, nxt)

    def total_copy(t):
        return remote(PART, TOT, fss.at[t], fsr, (t, p))

    @pl.when(active)
    def _():
        zero = jnp.zeros((comp, cells), F32)
        for e in E:
            e[nb + 2 * halo] = zero

            @pl.when(jnp.logical_not(has_slow))
            def _():
                for s in range(halo):
                    e[nb + slow_off + s] = zero

        SSV[halo] = zero
        for g in range(groups):
            ACC[pl.ds(g * 8, 8), :] = jnp.zeros((8, cells), F32)

        @pl.when(onpath)
        def _():
            for copy in coefficients(worker):
                copy.wait_recv()
            copy = pltpu.make_async_copy(IV, INTS, isem)
            copy.start()
            copy.wait()

            @pl.when(has_slow)
            def _():
                peer_ints(IV).start()

            @pl.when(self_a)
            def _():
                for copy in self_operands:
                    copy.wait()

            @pl.when(jnp.logical_not(self_a))
            def _():
                for copy in slab_operands(KA, SRCA, WA, ra, worker):
                    copy.wait_recv()

            pl.semaphore_signal(go_b, 1, device_id=home_b, device_id_type=MESH)
            pl.when(jnp.logical_not(odd))(send_even)
            halo_tables()
            prepare_slab(KA, LPA, LPMA, LBA, LAR, LHA)

            @pl.when(has_slow)
            def _():
                peer_face().start()
                peer_copy_a().start()
                for copy in (peer_ints(IV), peer_face(), peer_copy_a()):
                    copy.wait_recv()
                peer_tables()

        def take_b():
            for copy in slab_operands(KB, SRCB, WB, rb, worker):
                copy.wait_recv()
            prepare_slab(KB, LPB, LPMB, LBB, LBR, LHB)

            @pl.when(has_slow)
            def _():
                peer_copy_b().start()

        rushed = x == n_planes - 2
        pl.when(both(onpath, jnp.logical_not(rushed)))(take_b)

        @pl.when(both(native, has_slow))
        def _():
            peer_face().start()
            peer_copy_b().start()

        @pl.when(onpath)
        def _():
            run_slab(KA, SRCA, LPA, LPMA, LBA, LHA, PLHA, WA, OUTA, False, None)
            pl.when(rushed)(take_b)

        run_slab(KB, SRCB, LPB, LPMB, LBB, LHB, PLHB, WB, OUTB, True, onpath)

        early = both(onpath, jnp.logical_not(last))
        for i in range(PIECES):
            go_home(0, 0, i, early)

        PART[...] = jnp.sum(ACC[...].T, axis=0, keepdims=True)

        @pl.when(later)
        def _():
            part_copy().wait_recv()
            PART[...] = PART[...] + RED[...]

        @pl.when(more)
        def _():
            part_copy().start()

        @pl.when(last)
        def _():
            for t in range(n_tm):
                @pl.when(jnp.logical_not(same((t, p))))
                def _():
                    total_copy(t).start()

        for i in range(PIECES):
            go_home(1, 1, i, early)
            go_home(1, 0, i, early)
            go_home(0, 1, i, early)

    @pl.when(both(last, own_summer))
    def _():
        sens_o[...] = PART[...]

    @pl.when(jnp.logical_not(own_summer))
    def _():
        total_copy(0).wait_recv()
        sens_o[...] = TOT[...]

    @pl.when(last)
    def _():
        for t in range(n_tm):
            @pl.when(jnp.logical_not(same((t, p))))
            def _():
                total_copy(t).wait_send()

    @pl.when(more)
    def _():
        for i in range(CHUNKS):
            state_copy(i).wait_send()
        part_copy().wait_send()

    @pl.when(active)
    def _():
        fast_copy(0, (SWEEPS - 2) % 2, fast).wait_send()

    @pl.when(more)
    def _():
        fast_copy(0, (SWEEPS - 1) % 2, fast).wait_send()

    @pl.when(both(active, has_slow))
    def _():
        part_of_copy(0, slow).wait_send()
        peer_ints(IV).wait_send()
        peer_face().wait_send()
        peer_copy_b().wait_send()

    @pl.when(both(onpath, has_slow))
    def _():
        peer_copy_a().wait_send()

    @pl.when(both(more, has_slow))
    def _():
        whole_copy(0, slow).wait_send()

    for level in range(STEPS):
        for i in range(PIECES):
            go_home(1, level, i, onpath, True)
            go_home(0, level, i, onpath, True)
            stay(level, i, True)

    @pl.when(both(mover, odd, jnp.logical_not(own_worker)))
    def _():
        send_operands(KA, SRCA, WA, ra, True)

    @pl.when(both(mover, jnp.logical_not(odd)))
    def _():
        for copy in coefficients(worker):
            copy.wait_send()
        send_operands(KB, SRCB, WB, rb, True)

    @pl.when(relays)
    def _():
        onward_a, onward_b = operand_pieces(False)
        for i in range(comp + STEPS):
            pl.when(relay_a)(onward_a[i].wait_send)
            pl.when(relay_b)(onward_b[i].wait_send)

    @pl.when(both(mover, jnp.logical_not(own_worker)))
    def _():
        for level in range(STEPS):
            for i in range(PIECES):
                home_copy(0, level, i).wait_recv()


def per_device(source, terminal, jacobian, face_coef, cell_coef, neighbours, send_blocks,
               live_count, volume, shape_field, weights):
    nb, comp, cells = terminal.shape
    nei = face_coef.shape[1]
    halo = send_blocks.shape[2]
    anys = pl.BlockSpec(memory_space=pl.ANY)
    smem = pl.BlockSpec(memory_space=pltpu.SMEM)
    vmem = pltpu.VMEM
    dma = pltpu.SemaphoreType.DMA
    table = nb + 2 * halo + 1
    ints = jnp.concatenate(
        [
            neighbours.T.reshape(nei * nb),
            send_blocks[0, 0],
            send_blocks[0, 1],
            live_count,
            jnp.zeros(((8 - nei) * nb - 2 * halo - 1,), jnp.int32),
        ]
    )
    slab = vmem((comp, nb, cells), F32)
    plane = vmem((nb, cells), F32)
    rows8 = vmem((nb, 8, cells), F32)
    adj, sens = pl.pallas_call(
        kernel,
        out_shape=(
            jax.ShapeDtypeStruct((STEPS, comp, nb, cells), F32),
            jax.ShapeDtypeStruct((1, nb), F32),
        ),
        in_specs=[anys] * 8 + [smem],
        out_specs=(anys, pl.BlockSpec(memory_space=pltpu.VMEM)),
        scratch_shapes=[
            vmem((comp, comp, nb, cells), F32),
            vmem((comp, comp, nb, cells), F32),
            vmem((STEPS, comp, nb, cells), F32),
            vmem((STEPS, comp, nb, cells), F32),
            vmem((nei, nb, cells), F32),
            plane, plane, plane, plane,
            slab,
            slab, slab, slab, slab,
            rows8, rows8,
            slab, slab,
            rows8, rows8,
            vmem((table, comp, cells), F32),
            vmem((table, comp, cells), F32),
            vmem((table, comp, cells), F32),
            vmem((3, halo, comp, cells), F32),
            vmem((3, halo, comp, cells), F32),
            vmem((halo + 1, comp, cells), F32),
            vmem((halo, comp, cells), F32),
            vmem((2, halo, comp, cells), F32),
            vmem((STEPS, comp, nb, cells), F32),
            vmem((STEPS, comp, nb, cells), F32),
            plane,
            vmem((1, nb), F32),
            vmem((1, nb), F32),
            vmem((1, nb), F32),
            vmem((STEPS, 1, cells), F32),
            vmem((STEPS, 1, cells), F32),
            vmem((STEPS, 1, cells), F32),
            vmem((8 * nb,), jnp.int32),
            pltpu.SMEM((8 * nb,), jnp.int32),
            vmem((nei, 2 * halo, cells), F32),
            vmem((2 * halo, 8, cells), F32),
            vmem((2 * halo, 8, cells), F32),
            pltpu.SMEM((2 * halo * nei,), jnp.int32),
            pltpu.SMEM((halo * nei,), jnp.int32),
            vmem((8 * nb,), jnp.int32),
            pltpu.SMEM((8 * nb,), jnp.int32),
            vmem((nei, halo, cells), F32),
            vmem((halo, 8, cells), F32),
            vmem((halo, 8, cells), F32),
            pltpu.SMEM((halo * nei,), jnp.int32),
            dma((3,)),
            dma((3,)),
            dma((3,)),
            dma((5,)),
            dma((5,)),
            dma((comp + STEPS,)),
            dma((comp + STEPS,)),
            dma((comp + STEPS,)),
            pltpu.SemaphoreType.REGULAR,
            dma(()),
            dma((CHUNKS,)),
            dma((SLOTS,)),
            dma((3,)),
            dma((3,)),
            dma((2,)),
            dma(()),
            dma(()),
            dma((4,)),
            dma((4,)),
            dma((STEPS, PIECES)),
            dma((STEPS, PIECES)),
            dma((STEPS, PIECES)),
            dma((CHUNKS,)),
            dma(()),
            dma(()),
            dma((lax.axis_size("tm"),)),
            dma(()),
        ],
        compiler_params=pltpu.CompilerParams(collective_id=0, has_side_effects=True),
        name="sweep",
    )(
        source.transpose(0, 2, 1, 3),
        terminal.transpose(1, 0, 2),
        jacobian.transpose(0, 2, 3, 1, 4),
        face_coef.transpose(1, 0, 2),
        cell_coef,
        ints,
        volume,
        shape_field.transpose(1, 0, 2),
        weights,
    )
    return adj.transpose(0, 2, 1, 3), sens.reshape(nb)


def solution(mesh):
    return jax.shard_map(
        per_device,
        mesh=mesh,
        in_specs=(
            P("tm", "space", None, None),
            P("space", None, None),
            P("tm", "space", None, None, None),
            P("space", None, None),
            P("space", None),
            P("space", None),
            P("space", None, None),
            P("space"),
            P("space", None),
            P("space", None, None),
            P("tm"),
        ),
        out_specs=(P("tm", "space", None, None), P("space")),
        check_vma=False,
    )
```
